32 devices in a mesh: dp: 16 (over z, y, core), space: 2 (over x).
Axes of the slice: x: 2, y: 2, z: 4, core: 2. Of those that a mesh axis runs over, the one named last changes fastest.
Arguments:
- images: bfloat16 [16, 3, 512, 512], P('dp', None, 'space'), may hold values from -6 to 6
- pos_embed: bfloat16 [1024, 1280], P('space'), may hold values from -3 to 3
- conv_first: bfloat16 [3, 3, 3, 64], replicated, may hold values from -1.75 to 1.75
- conv_second: bfloat16 [3, 3, 64, 128], replicated, may hold values from -0.375 to 0.375
- conv_third: bfloat16 [3, 3, 128, 256], replicated, may hold values from -0.25 to 0.25
- conv_fourth: bfloat16 [3, 3, 256, 512], replicated, may hold values from -0.1875 to 0.1875
- proj_weight: bfloat16 [512, 1280], replicated, may hold values from -0.375 to 0.375
- ln_first: float32 [1280], replicated, may hold values from 0.25 to 1.75
- qkv_weight: bfloat16 [1280, 3, 1280], P('dp', None, 'space'), as said below
- out_weight: bfloat16 [1280, 1280], P('space', 'dp'), may hold values from -0.15625 to 0.15625
- ln_second: float32 [1280], replicated, may hold values from 0.25 to 1.75
- up_weight: bfloat16 [1280, 5120], P('dp', 'space'), may hold values from -0.15625 to 0.15625
- down_weight: bfloat16 [5120, 1280], P('space', 'dp'), may hold values from -0.125 to 0.125
Outputs:
- encoded: bfloat16 [16, 1024, 1280], P('dp', 'space')
The draws below stay inside these ranges and needn't reach their ends.
Inputs may be any that keep to these rules, and one draw needn't show every extreme that they name: `qkv_weight`: every entry is at most 135 * 1280 ** -0.5 in magnitude.
All inputs are finite; a program needn't handle non-finite values.
Results may differ from the reference program's by a relative error of at most 0.014.
Values may be sent and summed in bfloat16 or wider, within the bound.
A program may use at most 128 MiB of HBM per device.

```python
import jax
import jax.numpy as jnp
from jax import lax

D = 1280
HEADS = 16
FF = 5120
C1 = 64
C2 = 128
C3 = 256
C4 = 512
RES = 512
TOKS = 1024
IMAGES = 16
N_SPACE = 2


def draw_qkv_weight(key, part):
    first = jax.random.fold_in(jax.random.fold_in(key, 7), 0)
    base = jnp.clip(jax.random.normal(first, (D, 3, D), jnp.float32), -4.5, 4.5) / jnp.sqrt(jnp.float32(D))
    return base.astype(jnp.bfloat16)


def block_levels(own_key, shape, cuts, smallest, high):
    level, own = 1.0, jax.random.fold_in(own_key, 6)
    for position, blocks in cuts:
        draws = jnp.exp(jax.random.uniform(jax.random.fold_in(own, position), (blocks,), jnp.float32, smallest / len(cuts), high / len(cuts)))
        level = level * jnp.repeat(draws, shape[position] // blocks).reshape([-1 if axis == position else 1 for axis in range(len(shape))])
    return level


def bell_draw(rng, shape, scale, reach, pieces=(), dtype=jnp.bfloat16):
    level = block_levels(rng, shape, pieces, -0.22, 0.18) if pieces else 1.0
    entries = jax.random.normal(rng, shape, jnp.float32) * scale * level
    return jnp.minimum(jnp.maximum(entries, -reach), reach).astype(dtype)


def setup_inputs(seed: int = 0) -> dict:
    splits = jax.random.split(jax.random.key(seed), 14)
    return {
        "images": bell_draw(splits[0], (IMAGES, 3, RES, RES), 1.0, 6.0, ((0, 16), (2, 2))),
        "pos_embed": bell_draw(splits[1], (TOKS, D), 0.5, 3.0, ((0, 2),)),
        "conv_first": bell_draw(splits[2], (3, 3, 3, C1), 13 ** -0.5, 1.75),
        "conv_second": bell_draw(splits[3], (3, 3, C1, C2), (4 * C1) ** -0.5, 0.375),
        "conv_third": bell_draw(splits[4], (3, 3, C2, C3), (4 * C2) ** -0.5, 0.25),
        "conv_fourth": bell_draw(splits[5], (3, 3, C3, C4), (4 * C3) ** -0.5, 0.1875),
        "proj_weight": bell_draw(splits[6], (C4, D), (C4 // 2) ** -0.5, 0.375),
        "ln_first": jnp.clip(1.0 + 0.15 * jax.random.normal(splits[7], (D,), jnp.float32), 0.25, 1.75),
        "qkv_weight": draw_qkv_weight(jax.random.fold_in(splits[13], 71), 0),
        "out_weight": bell_draw(splits[9], (D, D), D ** -0.5, 0.15625, ((0, 2), (1, 16))),
        "ln_second": jnp.clip(1.0 + 0.15 * jax.random.normal(splits[10], (D,), jnp.float32), 0.25, 1.75),
        "up_weight": bell_draw(splits[11], (D, FF), D ** -0.5, 0.15625, ((0, 16), (1, 2))),
        "down_weight": bell_draw(splits[12], (FF, D), (FF // 2) ** -0.5, 0.125, ((0, 2), (1, 16))),
    }


def conv_layer(image_field, kernel, spec):
    out = lax.conv_general_dilated(image_field, kernel, (2, 2), ((1, 1), (1, 1)), dimension_numbers=spec, preferred_element_type=jnp.float32)
    return jax.nn.relu(out).astype(jnp.bfloat16)

def layer_norm(values, gain):
    wide = values.astype(jnp.float32)
    center = wide - lax.optimization_barrier(jnp.mean(wide, axis=-1, keepdims=True))
    spread = lax.optimization_barrier(jnp.mean(center * center, axis=-1, keepdims=True))
    return (center * lax.rsqrt(spread + 1e-06) * gain.astype(jnp.float32)).astype(jnp.bfloat16)

def softmax_mix(query, keys, values):
    head_size = query.shape[-1]
    scores = jnp.einsum('qhd,khd->hqk', query.astype(jnp.float32), keys.astype(jnp.float32)) / jnp.sqrt(jnp.float32(head_size))
    weights = jax.nn.softmax(scores, axis=-1).astype(jnp.bfloat16)
    return jnp.einsum('hqk,khd->qhd', weights.astype(jnp.float32), values.astype(jnp.float32)).astype(jnp.bfloat16)

def block_sum(left, right):
    inner = left.shape[1] // N_SPACE
    left_blocks = left.reshape(left.shape[0], N_SPACE, inner).astype(jnp.float32)
    right_blocks = right.reshape(N_SPACE, inner, right.shape[1]).astype(jnp.float32)
    parts = jnp.einsum('tsk,skd->std', left_blocks, right_blocks).astype(jnp.bfloat16)
    parts = lax.optimization_barrier(parts)
    return lax.optimization_barrier(jnp.sum(parts.astype(jnp.float32), axis=0))

def reference(images, pos_embed, conv_first, conv_second, conv_third, conv_fourth, proj_weight, ln_first, qkv_weight, out_weight, ln_second, up_weight, down_weight):

    def one_image(picture):
        stem_out = conv_layer(picture[None], conv_first, ('NCHW', 'HWIO', 'NHWC'))
        for kernel in (conv_second, conv_third, conv_fourth):
            stem_out = conv_layer(stem_out, kernel, ('NHWC', 'HWIO', 'NHWC'))
        flat = stem_out.reshape(TOKS, C4)
        tokens = (jnp.dot(flat, proj_weight, preferred_element_type=jnp.float32) + pos_embed.astype(jnp.float32)).astype(jnp.bfloat16)
        normed = layer_norm(tokens, ln_first)
        qkv = jnp.dot(normed, qkv_weight.reshape(D, 3 * D), preferred_element_type=jnp.float32).astype(jnp.bfloat16)
        qkv = qkv.reshape(TOKS, 3, HEADS, D // HEADS)
        mixed = softmax_mix(qkv[:, 0], qkv[:, 1], qkv[:, 2]).reshape(TOKS, D)
        after_attn = (tokens.astype(jnp.float32) + block_sum(mixed, out_weight)).astype(jnp.bfloat16)
        normed_two = layer_norm(after_attn, ln_second)
        hidden = jax.nn.gelu(jnp.dot(normed_two, up_weight, preferred_element_type=jnp.float32), approximate=False).astype(jnp.bfloat16)
        encoded = after_attn.astype(jnp.float32) + block_sum(hidden, down_weight)
        return encoded.astype(jnp.bfloat16)
    return lax.map(one_image, images)
```

```python
import functools
import math

import jax
import jax.numpy as jnp
from jax import lax
from jax.experimental import pallas as pl
from jax.experimental.pallas import tpu as pltpu
from jax.sharding import PartitionSpec as P

HEADS = 16
PHASES = 5


def passed_along(value, axis, steps):
    count = lax.axis_size(axis)
    leading, last = (max(0, -steps), min(count, count - steps))
    return lax.ppermute(value, axis, [(source, source + steps) for source in range(leading, last)])


def shifted(value, axis, steps):
    count = lax.axis_size(axis)
    return lax.ppermute(value, axis, [(source, (source + steps) % count) for source in range(count)])


def largest_divisor(number, limit):
    return max(d for d in range(1, limit + 1) if number % d == 0)


def first_conv_body(unroll, field_ref, kernel_ref, out_ref):
    depth = field_ref.shape[1]
    lanes = field_ref.shape[2]

    def step(index, carry):
        for part in range(unroll):
            row = index * unroll + part
            patch = field_ref[pl.ds(2 * row, 3)].reshape(3 * depth, lanes)
            out = lax.dot_general(
                patch, kernel_ref[...], (((0,), (0,)), ((), ())), preferred_element_type=jnp.float32
            )
            out_ref[row] = jnp.maximum(out, 0.0).astype(out_ref.dtype)
        return carry

    lax.fori_loop(0, out_ref.shape[0] // unroll, step, 0)


def first_conv(images, margin, kernel):
    wide = images.shape[3]
    pairs = wide // 4
    channels = images.shape[1]
    out_channels = kernel.shape[3]
    source = lax.broadcasted_iota(jnp.int32, (wide, PHASES, pairs), 0)
    phase = lax.broadcasted_iota(jnp.int32, (wide, PHASES, pairs), 1)
    pair = lax.broadcasted_iota(jnp.int32, (wide, PHASES, pairs), 2)
    pick = (source == 4 * pair + phase - 1).astype(jnp.bfloat16)
    field = jnp.concatenate([margin, images], axis=2)[0]
    rows = field.shape[1]
    picked = jnp.einsum("chw,wqp->hcqp", field, pick, preferred_element_type=jnp.float32)
    picked = picked.astype(jnp.bfloat16).reshape(rows, channels * PHASES, pairs)
    depth = -(-channels * PHASES // 16) * 16
    picked = jnp.pad(picked, ((0, 0), (0, depth - channels * PHASES), (0, 0)))
    taps = jnp.transpose(kernel, (0, 2, 1, 3))
    left = jnp.pad(taps, ((0, 0), (0, 0), (0, 2), (0, 0)))
    right = jnp.pad(taps, ((0, 0), (0, 0), (2, 0), (0, 0)))
    both = jnp.concatenate([left, right], axis=3).reshape(3, channels * PHASES, 2 * out_channels)
    both = jnp.pad(both, ((0, 0), (0, depth - channels * PHASES), (0, 0)))
    both = both.reshape(3 * depth, 2 * out_channels)
    count = (rows - 3) // 2 + 1
    out = pl.pallas_call(
        functools.partial(first_conv_body, largest_divisor(count, 16)),
        out_shape=jax.ShapeDtypeStruct((count, pairs, 2 * out_channels), jnp.bfloat16),
        in_specs=[pl.BlockSpec(memory_space=pltpu.VMEM)] * 2,
        out_specs=pl.BlockSpec(memory_space=pltpu.VMEM),
        compiler_params=pltpu.CompilerParams(vmem_limit_bytes=40 * 1024 * 1024),
        cost_estimate=pl.CostEstimate(
            flops=count * pairs * depth * 3 * 4 * out_channels * 4,
            bytes_accessed=count * pairs * out_channels * 4,
            transcendentals=0,
        ),
    )(picked, both)
    return out[None]


def second_conv(field, kernel):
    height, _, inner, outer = kernel.shape
    before = jnp.concatenate([jnp.zeros_like(kernel[:, 0]), kernel[:, 0]], axis=1)
    here = jnp.concatenate([kernel[:, 1], kernel[:, 2]], axis=1)
    paired = jnp.stack([before, here], axis=1)
    out = lax.conv_general_dilated(
        field,
        paired,
        (2, 1),
        ((0, 0), (1, 0)),
        dimension_numbers=("NHWC", "HWIO", "NHWC"),
        preferred_element_type=jnp.float32,
    )
    return jax.nn.relu(out).astype(jnp.bfloat16)


def later_conv(field, kernel):
    out = lax.conv_general_dilated(
        field,
        kernel,
        (2, 2),
        ((0, 0), (1, 1)),
        dimension_numbers=("NHWC", "HWIO", "NHWC"),
        preferred_element_type=jnp.float32,
    )
    return jax.nn.relu(out).astype(jnp.bfloat16)


def layer_norm(values, gain):
    wide = values.astype(jnp.float32)
    center = wide - jnp.mean(wide, axis=-1, keepdims=True)
    spread = jnp.mean(center * center, axis=-1, keepdims=True)
    return (center * lax.rsqrt(spread + 1e-06) * gain).astype(jnp.bfloat16)


def attend_body(chunks, factor, *refs):
    query_ref, out_ref = refs[0], refs[-1]
    keys, values = refs[1 : 1 + chunks], refs[1 + chunks : 1 + 2 * chunks]
    total = query_ref.shape[1]
    block = largest_divisor(total // 128, 2) * 128
    for start in range(0, total, block):
        query = query_ref[:, start : start + block]
        scores = [
            lax.dot_general(
                key[...], query, (((0,), (0,)), ((), ())), preferred_element_type=jnp.float32
            )
            for key in keys
        ]
        top = functools.reduce(
            jnp.maximum, [jnp.max(score, axis=0, keepdims=True) for score in scores]
        )
        weights = [jnp.exp2((score - top) * factor) for score in scores]
        below = sum(jnp.sum(weight, axis=0, keepdims=True) for weight in weights)
        mixed = sum(
            jnp.dot(value[...], weight.astype(jnp.bfloat16), preferred_element_type=jnp.float32)
            for value, weight in zip(values, weights)
        )
        out_ref[:, start : start + block] = (mixed / below).astype(out_ref.dtype)


def attend(query, keys, values, head_size):
    local, total = query.shape
    chunks = len(keys)
    seen = sum(key.shape[1] for key in keys)
    spec = lambda array: pl.BlockSpec((head_size, array.shape[1]), lambda head: (head, 0))
    factor = math.log2(math.e) / math.sqrt(head_size)
    return pl.pallas_call(
        functools.partial(attend_body, chunks, factor),
        grid=(local // head_size,),
        out_shape=jax.ShapeDtypeStruct((local, total), jnp.bfloat16),
        in_specs=[spec(array) for array in (query, *keys, *values)],
        out_specs=spec(query),
        compiler_params=pltpu.CompilerParams(vmem_limit_bytes=40 * 1024 * 1024),
        cost_estimate=pl.CostEstimate(
            flops=local * total * seen * 16,
            bytes_accessed=local * (2 * total + 2 * seen) * 2,
            transcendentals=(local // head_size) * total * seen,
        ),
    )(query, *keys, *values)


def gathered(weight, axis):
    return lax.all_gather(weight, "dp", axis=axis, tiled=True)


MESH = pl.DeviceIdType.MESH
VMEM_LIMIT = 62 * 1024 * 1024


def norm_rows(values, gain):
    wide = values.astype(jnp.float32)
    center = wide - jnp.mean(wide, axis=-1, keepdims=True)
    spread = jnp.mean(center * center, axis=-1, keepdims=True)
    return (center * lax.rsqrt(spread + 1e-06) * gain).astype(jnp.bfloat16)


def pair_dot(left, right, dims):
    return lax.dot_general(left, right, (dims, ((), ())), preferred_element_type=jnp.float32)


class Gather:
    def __init__(self, number, line, place, source, at, both, sems):
        self.number, self.line, self.source, self.at, self.both = number, line, source, at, both
        self.z, self.y, self.core, self.zpeers, self.ypeer, self.sibling = place
        self.zsend, self.zrecv, self.ysend, self.yrecv, self.csend, self.crecv, self.local = sems

    def copy(self, source, target, send, recv, device):
        return pltpu.make_async_remote_copy(
            src_ref=source, dst_ref=target, send_sem=send, recv_sem=recv,
            device_id=device, device_id_type=MESH,
        )

    def own_copy(self):
        mine = self.at(self.z, self.y, self.core)
        return pltpu.make_async_copy(self.source, mine, self.local.at[self.number])

    def z_copy(self, step):
        mine = self.at(self.z, self.y, self.core)
        return self.copy(
            self.source, mine, self.zsend.at[self.number, step],
            self.zrecv.at[self.number, self.z], self.zpeers[step],
        )

    def y_own(self):
        mine = self.at(self.z, self.y, self.core)
        return self.copy(
            self.source, mine, self.ysend.at[self.number, self.z],
            self.yrecv.at[self.number, self.z], self.ypeer,
        )

    def y_copy(self, slab, row):
        here = self.at(slab, row, self.core)
        return self.copy(
            here, here, self.ysend.at[self.number, slab], self.yrecv.at[self.number, slab], self.ypeer
        )

    def core_copy(self, slab, core):
        here = self.both(slab, core)
        return self.copy(
            here, here, self.csend.at[self.number, slab], self.crecv.at[self.number, slab], self.sibling
        )

    def start(self):
        self.own_copy().start()
        for step in range(1, self.line):
            self.z_copy(step).start()

    def start_y(self):
        self.y_own().start()

    def forward(self, slab):
        @pl.when(slab != self.z)
        def _():
            here = self.at(slab, self.y, self.core)
            self.copy(
                here, here, self.zsend.at[self.number, 0], self.zrecv.at[self.number, slab], self.ypeer
            ).wait_recv()
            self.y_copy(slab, self.y).start()

    def mirror(self, slab):
        @pl.when(slab == self.z)
        def _():
            self.own_copy().wait()

        self.y_copy(slab, 1 - self.y).wait_recv()
        self.core_copy(slab, self.core).start()

    def ready(self, slab):
        self.core_copy(slab, 1 - self.core).wait_recv()

    def drain(self):
        for step in range(1, self.line):
            self.z_copy(step).wait_send()
        for slab in range(self.line):
            self.y_copy(slab, self.y).wait_send()
            self.core_copy(slab, self.core).wait_send()


def block_body(
    line, head_size,
    flat_in, pos_in, proj, gain_one, gain_two, qkv_in, out_in, up_in, down_in,
    encoded,
    flat, pos, tokens, normed, wqkv, wout, wout_other, wup, wdown, qkv, mixed, hidden, total, back, arrived,
    zsend, zrecv, ysend, yrecv, csend, crecv, local, misc_send, misc_recv, misc_local, mix_send, mix_recv, back_send, back_recv,
):
    me, side = lax.axis_index("dp"), lax.axis_index("space")
    other = 1 - side
    core = me % 2
    y = (me // 2) % 2
    z = me // 4
    sibling = {"dp": me + 1 - 2 * core, "space": side}
    ypeer = {"dp": me + 2 - 4 * y, "space": side}
    xpeer = {"dp": me, "space": other}
    zpeers = [None] + [
        {"dp": ((z + step) % line) * 4 + y * 2 + core, "space": side} for step in range(1, line)
    ]

    barrier = pltpu.get_barrier_semaphore()
    greeted = [sibling, ypeer, xpeer] + zpeers[1:]
    for device in greeted:
        pl.semaphore_signal(barrier, inc=1, device_id=device, device_id_type=MESH)
    pl.semaphore_wait(barrier, len(greeted))

    def remote(source, target, slot, device):
        return pltpu.make_async_remote_copy(
            src_ref=source, dst_ref=target, send_sem=misc_send.at[slot], recv_sem=misc_recv.at[slot],
            device_id=device, device_id_type=MESH,
        )

    place = (z, y, core, zpeers, ypeer, sibling)
    sems = (zsend, zrecv, ysend, yrecv, csend, crecv, local)

    def gather(number, source, at, both):
        return Gather(number, line, place, source, at, both, sems)

    g_out = gather(0, out_in, lambda a, b, c: wout.at[a, b, c], lambda a, c: wout.at[a, :, c])
    g_qkv = gather(1, qkv_in, lambda a, b, c: wqkv.at[:, a, b, c], lambda a, c: wqkv.at[:, a, :, c])
    g_up = gather(2, up_in, lambda a, b, c: wup.at[a, b, c], lambda a, c: wup.at[a, :, c])
    g_down = gather(3, down_in, lambda a, b, c: wdown.at[a, b, c], lambda a, c: wdown.at[a, :, c])
    gathers = [g_out, g_qkv, g_up, g_down]

    rows = flat_in.shape[0]
    half = rows // 2
    width = proj.shape[1]
    heads = qkv.shape[1]
    count = 2 * rows

    flat_send = remote(flat_in, flat.at[side], 0, xpeer)
    flat_send.start()
    piece = pl.ds(core * half, half)
    other_piece = pl.ds((1 - core) * half, half)
    pos_send = remote(pos_in.at[piece], pos.at[side, piece], 1, xpeer)
    pos_send.start()
    pos_own = pltpu.make_async_copy(pos_in, pos.at[side], misc_local.at[0])
    pos_own.start()
    for g in gathers:
        g.start()
    g_out.start_y()
    g_qkv.start_y()

    def embed(source, where, first):
        own = pl.ds(first, half)
        chunk = (
            jnp.dot(source[own], proj[...], preferred_element_type=jnp.float32)
            + pos[where, own].astype(jnp.float32)
        ).astype(jnp.bfloat16)
        tokens[where, own] = chunk
        normed[where, own] = norm_rows(chunk, gain_one[...])

    pos_own.wait()
    embed(flat_in, side, 0)
    for slab in range(line):
        g_out.forward(slab)
    embed(flat_in, side, half)
    for slab in range(line):
        g_qkv.forward(slab)
    for slab in range(line):
        g_out.mirror(slab)
    out_cross = remote(wout.at[:, :, core], wout_other.at[:, :, core], 2, xpeer)
    out_cross.start()
    remote(pos.at[other, piece], pos.at[other, piece], 1, xpeer).wait_recv()
    pos_mirror = remote(pos.at[other, piece], pos.at[other, piece], 3, sibling)
    pos_mirror.start()
    remote(flat.at[other], flat.at[other], 0, xpeer).wait_recv()
    remote(pos.at[other, other_piece], pos.at[other, other_piece], 3, sibling).wait_recv()
    embed(flat.at[other], other, 0)
    embed(flat.at[other], other, half)
    g_up.start_y()
    for slab in range(line):
        g_qkv.mirror(slab)
    for slab in range(line):
        g_qkv.ready(slab)

    def project(step, carry):
        which, where = step // 2, step % 2
        weight = wqkv[which].reshape(width, heads * head_size)
        made = pair_dot(weight, normed[where], ((0,), (1,)))
        columns = pl.ds(pl.multiple_of(where * rows, rows), rows)
        qkv[which, :, :, columns] = made.astype(jnp.bfloat16).reshape(heads, head_size, rows)
        return carry

    lax.fori_loop(0, 6, project, 0)

    factor = math.log2(math.e) / math.sqrt(head_size)
    block = largest_divisor(count // 128, 2) * 128

    def attend_head(head, carry):
        keys, values = qkv[1, head], qkv[2, head]
        for start in range(0, count, block):
            query = qkv[0, head, :, start : start + block]
            score = pair_dot(keys, query, ((0,), (0,)))
            top = jnp.max(score, axis=0, keepdims=True)
            weight = jnp.exp2((score - top) * factor)
            below = jnp.sum(weight, axis=0, keepdims=True)
            made = jnp.dot(values, weight.astype(jnp.bfloat16), preferred_element_type=jnp.float32)
            mixed[side, head, :, start : start + block] = (made / below).astype(jnp.bfloat16)
        mix_copy(side, head).start()

        @pl.when(head < line)
        def _():
            g_up.forward(head)

        return carry

    def mix_copy(where, head):
        return pltpu.make_async_remote_copy(
            src_ref=mixed.at[where, head], dst_ref=mixed.at[where, head],
            send_sem=mix_send.at[head], recv_sem=mix_recv.at[head], device_id=xpeer, device_id_type=MESH,
        )

    lax.fori_loop(0, heads, attend_head, 0)

    cross = wout_other.at[:, :, core]
    remote(cross, cross, 2, xpeer).wait_recv()
    out_mirror = remote(cross, cross, 4, sibling)
    out_mirror.start()
    g_down.start_y()
    for slab in range(line):
        g_out.ready(slab)
    for slab in range(line):
        g_up.mirror(slab)
    cross_other = wout_other.at[:, :, 1 - core]
    remote(cross_other, cross_other, 4, sibling).wait_recv()
    for head in range(heads):
        mix_copy(other, head).wait_recv()

    def settle(step, carry):
        where, first = step // 2, pl.multiple_of((step % 2) * half, half)
        columns = pl.ds(pl.multiple_of(step * half, half), half)
        own = pl.ds(first, half)
        attn = tokens[where, own].astype(jnp.float32)
        for part, weight in ((side, wout), (other, wout_other)):
            left = mixed[part, :, :, columns].reshape(heads * head_size, half)
            share = pair_dot(left, weight[...].reshape(width, heads * head_size), ((0,), (1,)))
            attn = attn + share.astype(jnp.bfloat16).astype(jnp.float32)
        chunk = attn.astype(jnp.bfloat16)
        tokens[where, own] = chunk
        normed[where, own] = norm_rows(chunk, gain_two[...])
        return carry

    lax.fori_loop(0, 4, settle, 0)
    for slab in range(line):
        g_down.forward(slab)
    for slab in range(line):
        g_up.ready(slab)

    units = hidden.shape[2]
    part = units // 4

    def rise(step, carry):
        where, first = step // 4, pl.multiple_of((step % 4) * part, part)
        weight = wup[:, :, :, :, pl.ds(first, part)].reshape(width, part)
        before = jnp.dot(normed[where], weight, preferred_element_type=jnp.float32)
        made = 0.5 * before * (1.0 + lax.erf(before * math.sqrt(0.5)))
        hidden[where, :, pl.ds(first, part)] = made.astype(jnp.bfloat16)
        return carry

    lax.fori_loop(0, 8, rise, 0)

    slab_rows = width // line

    def back_copy(slab):
        there = pl.ds(pl.multiple_of(slab * slab_rows, slab_rows), slab_rows)
        return pltpu.make_async_remote_copy(
            src_ref=back.at[there], dst_ref=arrived.at[there],
            send_sem=back_send.at[slab], recv_sem=back_recv.at[slab], device_id=xpeer, device_id_type=MESH,
        )

    for slab in range(line):
        g_down.mirror(slab)

    def fall(slab, carry):
        g_down.ready(slab)
        there = pl.ds(pl.multiple_of(slab * slab_rows, slab_rows), slab_rows)
        weight = wdown[slab].reshape(slab_rows, units)
        back[there] = pair_dot(weight, hidden[other], ((1,), (1,))).astype(jnp.bfloat16)
        back_copy(slab).start()
        total[there] = pair_dot(weight, hidden[side], ((1,), (1,))).astype(jnp.bfloat16)
        return carry

    lax.fori_loop(0, line, fall, 0)
    for slab in range(line):
        back_copy(slab).wait_recv()
    summed = total[...].astype(jnp.float32) + arrived[...].astype(jnp.float32)
    encoded[...] = (tokens[side].astype(jnp.float32) + summed.T).astype(jnp.bfloat16)

    flat_send.wait_send()
    pos_send.wait_send()
    out_cross.wait_send()
    pos_mirror.wait_send()
    out_mirror.wait_send()
    for head in range(heads):
        mix_copy(side, head).wait_send()
    for slab in range(line):
        back_copy(slab).wait_send()
    for g in gathers:
        g.drain()


def encoder_block(flat, pos, proj, gain_one, gain_two, qkv_shard, out_shard, up_shard, down_shard):
    shards = lax.axis_size("dp")
    line = shards // 4
    depth = qkv_shard.shape[1]
    local = qkv_shard.shape[2]
    units = up_shard.shape[1]
    rows = flat.shape[0]
    width = proj.shape[1]
    head_size = width // HEADS
    heads = local // head_size
    here = (line, 2, 2, depth)
    bf16 = jnp.bfloat16
    vmem = pl.BlockSpec(memory_space=pltpu.VMEM)
    hbm = pl.BlockSpec(memory_space=pl.ANY)
    dma = pltpu.SemaphoreType.DMA
    return pl.pallas_call(
        functools.partial(block_body, line, head_size),
        out_shape=jax.ShapeDtypeStruct((rows, width), bf16),
        in_specs=[vmem, hbm, vmem, vmem, vmem, hbm, hbm, hbm, hbm],
        out_specs=vmem,
        scratch_shapes=[
            pltpu.VMEM((2, rows, flat.shape[1]), bf16),
            pltpu.VMEM((2, rows, width), bf16),
            pltpu.VMEM((2, rows, width), bf16),
            pltpu.VMEM((2, rows, width), bf16),
            pltpu.VMEM((3, *here, local), bf16),
            pltpu.VMEM((*here, local), bf16),
            pltpu.VMEM((*here, local), bf16),
            pltpu.VMEM((*here, units), bf16),
            pltpu.VMEM((*here, units), bf16),
            pltpu.VMEM((3, heads, head_size, 2 * rows), bf16),
            pltpu.VMEM((2, heads, head_size, 2 * rows), bf16),
            pltpu.VMEM((2, rows, units), bf16),
            pltpu.VMEM((width, rows), bf16),
            pltpu.VMEM((width, rows), bf16),
            pltpu.VMEM((width, rows), bf16),
            dma((4, line)),
            dma((4, line)),
            dma((4, line)),
            dma((4, line)),
            dma((4, line)),
            dma((4, line)),
            dma((4,)),
            dma((5,)),
            dma((5,)),
            dma((1,)),
            dma((heads,)),
            dma((heads,)),
            dma((line,)),
            dma((line,)),
        ],
        compiler_params=pltpu.CompilerParams(
            collective_id=0, has_side_effects=True, vmem_limit_bytes=VMEM_LIMIT
        ),
    )(
        flat, pos, proj, gain_one[None], gain_two[None], qkv_shard, out_shard, up_shard, down_shard
    )


def on_ring(
    images,
    pos_embed,
    conv_first,
    conv_second,
    conv_third,
    conv_fourth,
    proj_weight,
    ln_first,
    qkv_weight,
    out_weight,
    ln_second,
    up_weight,
    down_weight,
):
    count = lax.axis_size("space")
    attention_part = gathered(
        jnp.concatenate([jnp.moveaxis(qkv_weight, 1, 0), out_weight.T[None]], axis=0), 1
    )
    feed_part = gathered(jnp.stack([up_weight, down_weight.T]), 1)
    out_part = attention_part[3]
    up_part, down_part = feed_part[0], feed_part[1]
    margin = passed_along(images[:, :, -15:, :], "space", 1)
    positions = [pos_embed] + [shifted(pos_embed, "space", k) for k in range(1, count)]

    stem_out = second_conv(first_conv(images, margin, conv_first), conv_second)
    for kernel in (conv_third, conv_fourth):
        stem_out = later_conv(stem_out, kernel)
    flat = stem_out.reshape(-1, stem_out.shape[3])
    flats = [flat] + [shifted(flat, "space", k) for k in range(1, count)]
    width = proj_weight.shape[1]
    local = attention_part.shape[2]
    head_size = width // HEADS

    tokens = None
    projected = []
    for rows, position in zip(flats, positions):
        chunk = (
            jnp.dot(rows, proj_weight, preferred_element_type=jnp.float32)
            + position.astype(jnp.float32)
        ).astype(jnp.bfloat16)
        tokens = chunk if tokens is None else tokens
        normed = layer_norm(chunk, ln_first)
        projected.append(
            [
                lax.dot_general(
                    attention_part[which],
                    normed,
                    (((0,), (1,)), ((), ())),
                    preferred_element_type=jnp.float32,
                ).astype(jnp.bfloat16)
                for which in range(3)
            ]
        )
    keys = [part[1] for part in projected]
    values = [part[2] for part in projected]

    def attention_share(query):
        mixed = attend(query, keys, values, head_size)
        share = lax.dot_general(
            mixed, out_part, (((0,), (1,)), ((), ())), preferred_element_type=jnp.float32
        ).astype(jnp.bfloat16)
        return mixed, share

    returned = []
    last = None
    for k in list(range(1, count)) + [0]:
        query = projected[k][0]
        if last is not None:
            query, _ = lax.optimization_barrier((query, last))
        last, share = attention_share(query)
        returned.append(shifted(share, "space", -k) if k else share)
    attn_sum = sum(part.astype(jnp.float32) for part in returned)
    after_attn = (tokens.astype(jnp.float32) + attn_sum).astype(jnp.bfloat16)
    normed_two = layer_norm(after_attn, ln_second)

    def feed_forward(rows):
        before = jnp.dot(rows, up_part, preferred_element_type=jnp.float32)
        hidden = (0.5 * before * (1.0 + lax.erf(before * math.sqrt(0.5)))).astype(jnp.bfloat16)
        hidden = lax.optimization_barrier(hidden)
        return lax.dot_general(
            hidden, down_part, (((1,), (1,)), ((), ())), preferred_element_type=jnp.float32
        ).astype(jnp.bfloat16)

    rows = normed_two.shape[0]
    half = rows // 2
    pieces = [normed_two[:half], normed_two[half:]]
    moved = [[shifted(piece, "space", k) for piece in pieces] for k in range(1, count)]
    totals = feed_forward(normed_two).astype(jnp.float32)
    back = [
        jnp.concatenate([shifted(feed_forward(piece), "space", -k) for piece in there], axis=0)
        for k, there in zip(range(1, count), moved)
    ]
    for part in back:
        totals = totals + part.astype(jnp.float32)
    return (after_attn.astype(jnp.float32) + totals).astype(jnp.bfloat16)[None]


def stem(images, conv_first, conv_second, conv_third, conv_fourth):
    margin = passed_along(images[:, :, -15:, :], "space", 1)
    stem_out = second_conv(first_conv(images, margin, conv_first), conv_second)
    for kernel in (conv_third, conv_fourth):
        stem_out = later_conv(stem_out, kernel)
    return stem_out.reshape(-1, stem_out.shape[3])


def on_device(
    images,
    pos_embed,
    conv_first,
    conv_second,
    conv_third,
    conv_fourth,
    proj_weight,
    ln_first,
    qkv_weight,
    out_weight,
    ln_second,
    up_weight,
    down_weight,
):
    shards = lax.axis_size("dp")
    fits = lax.axis_size("space") == 2 and shards % 4 == 0 and HEADS % 2 == 0
    fits = fits and qkv_weight.shape[0] % 16 == 0 and qkv_weight.shape[2] % 128 == 0
    if not fits:
        return on_ring(
            images, pos_embed, conv_first, conv_second, conv_third, conv_fourth, proj_weight,
            ln_first, qkv_weight, out_weight, ln_second, up_weight, down_weight,
        )
    flat = stem(images, conv_first, conv_second, conv_third, conv_fourth)
    out = encoder_block(
        flat, pos_embed, proj_weight, ln_first, ln_second,
        jnp.moveaxis(qkv_weight, 1, 0), out_weight.T, up_weight, down_weight.T,
    )
    return out[None]


def solution(mesh):
    placed = (
        P("dp", None, "space", None),
        P("space", None),
        P(),
        P(),
        P(),
        P(),
        P(),
        P(),
        P("dp", None, "space"),
        P("space", "dp"),
        P(),
        P("dp", "space"),
        P("space", "dp"),
    )
    return jax.shard_map(
        on_device, mesh=mesh, in_specs=placed, out_specs=P("dp", "space", None), check_vma=False
    )
```

```python
import functools
import math

import jax
import jax.numpy as jnp
from jax import lax
from jax.experimental import pallas as pl
from jax.experimental.pallas import tpu as pltpu
from jax.sharding import PartitionSpec as P

HEADS = 16
PHASES = 5


def passed_along(value, axis, steps):
    count = lax.axis_size(axis)
    leading, last = (max(0, -steps), min(count, count - steps))
    return lax.ppermute(value, axis, [(source, source + steps) for source in range(leading, last)])


def shifted(value, axis, steps):
    count = lax.axis_size(axis)
    return lax.ppermute(value, axis, [(source, (source + steps) % count) for source in range(count)])


def largest_divisor(number, limit):
    return max(d for d in range(1, limit + 1) if number % d == 0)


def first_conv_body(unroll, field_ref, kernel_ref, out_ref):
    depth = field_ref.shape[1]
    lanes = field_ref.shape[2]

    def step(index, carry):
        for part in range(unroll):
            row = index * unroll + part
            patch = field_ref[pl.ds(2 * row, 3)].reshape(3 * depth, lanes)
            out = lax.dot_general(
                patch, kernel_ref[...], (((0,), (0,)), ((), ())), preferred_element_type=jnp.float32
            )
            out_ref[row] = jnp.maximum(out, 0.0).astype(out_ref.dtype)
        return carry

    lax.fori_loop(0, out_ref.shape[0] // unroll, step, 0)


def first_conv(images, margin, kernel):
    wide = images.shape[3]
    pairs = wide // 4
    channels = images.shape[1]
    out_channels = kernel.shape[3]
    source = lax.broadcasted_iota(jnp.int32, (wide, PHASES, pairs), 0)
    phase = lax.broadcasted_iota(jnp.int32, (wide, PHASES, pairs), 1)
    pair = lax.broadcasted_iota(jnp.int32, (wide, PHASES, pairs), 2)
    pick = (source == 4 * pair + phase - 1).astype(jnp.bfloat16)
    field = jnp.concatenate([margin, images], axis=2)[0]
    rows = field.shape[1]
    picked = jnp.einsum("chw,wqp->hcqp", field, pick, preferred_element_type=jnp.float32)
    picked = picked.astype(jnp.bfloat16).reshape(rows, channels * PHASES, pairs)
    depth = -(-channels * PHASES // 16) * 16
    picked = jnp.pad(picked, ((0, 0), (0, depth - channels * PHASES), (0, 0)))
    taps = jnp.transpose(kernel, (0, 2, 1, 3))
    left = jnp.pad(taps, ((0, 0), (0, 0), (0, 2), (0, 0)))
    right = jnp.pad(taps, ((0, 0), (0, 0), (2, 0), (0, 0)))
    both = jnp.concatenate([left, right], axis=3).reshape(3, channels * PHASES, 2 * out_channels)
    both = jnp.pad(both, ((0, 0), (0, depth - channels * PHASES), (0, 0)))
    both = both.reshape(3 * depth, 2 * out_channels)
    count = (rows - 3) // 2 + 1
    out = pl.pallas_call(
        functools.partial(first_conv_body, largest_divisor(count, 16)),
        out_shape=jax.ShapeDtypeStruct((count, pairs, 2 * out_channels), jnp.bfloat16),
        in_specs=[pl.BlockSpec(memory_space=pltpu.VMEM)] * 2,
        out_specs=pl.BlockSpec(memory_space=pltpu.VMEM),
        compiler_params=pltpu.CompilerParams(vmem_limit_bytes=40 * 1024 * 1024),
        cost_estimate=pl.CostEstimate(
            flops=count * pairs * depth * 3 * 4 * out_channels * 4,
            bytes_accessed=count * pairs * out_channels * 4,
            transcendentals=0,
        ),
    )(picked, both)
    return out[None]


def second_conv(field, kernel):
    height, _, inner, outer = kernel.shape
    before = jnp.concatenate([jnp.zeros_like(kernel[:, 0]), kernel[:, 0]], axis=1)
    here = jnp.concatenate([kernel[:, 1], kernel[:, 2]], axis=1)
    paired = jnp.stack([before, here], axis=1)
    out = lax.conv_general_dilated(
        field,
        paired,
        (2, 1),
        ((0, 0), (1, 0)),
        dimension_numbers=("NHWC", "HWIO", "NHWC"),
        preferred_element_type=jnp.float32,
    )
    return jax.nn.relu(out).astype(jnp.bfloat16)


def later_conv(field, kernel):
    out = lax.conv_general_dilated(
        field,
        kernel,
        (2, 2),
        ((0, 0), (1, 1)),
        dimension_numbers=("NHWC", "HWIO", "NHWC"),
        preferred_element_type=jnp.float32,
    )
    return jax.nn.relu(out).astype(jnp.bfloat16)


def layer_norm(values, gain):
    wide = values.astype(jnp.float32)
    center = wide - jnp.mean(wide, axis=-1, keepdims=True)
    spread = jnp.mean(center * center, axis=-1, keepdims=True)
    return (center * lax.rsqrt(spread + 1e-06) * gain).astype(jnp.bfloat16)


def attend_body(chunks, factor, *refs):
    query_ref, out_ref = refs[0], refs[-1]
    keys, values = refs[1 : 1 + chunks], refs[1 + chunks : 1 + 2 * chunks]
    total = query_ref.shape[1]
    block = largest_divisor(total // 128, 2) * 128
    for start in range(0, total, block):
        query = query_ref[:, start : start + block]
        scores = [
            lax.dot_general(
                key[...], query, (((0,), (0,)), ((), ())), preferred_element_type=jnp.float32
            )
            for key in keys
        ]
        top = functools.reduce(
            jnp.maximum, [jnp.max(score, axis=0, keepdims=True) for score in scores]
        )
        weights = [jnp.exp2((score - top) * factor) for score in scores]
        below = sum(jnp.sum(weight, axis=0, keepdims=True) for weight in weights)
        mixed = sum(
            jnp.dot(value[...], weight.astype(jnp.bfloat16), preferred_element_type=jnp.float32)
            for value, weight in zip(values, weights)
        )
        out_ref[:, start : start + block] = (mixed / below).astype(out_ref.dtype)


def attend(query, keys, values, head_size):
    local, total = query.shape
    chunks = len(keys)
    seen = sum(key.shape[1] for key in keys)
    spec = lambda array: pl.BlockSpec((head_size, array.shape[1]), lambda head: (head, 0))
    factor = math.log2(math.e) / math.sqrt(head_size)
    return pl.pallas_call(
        functools.partial(attend_body, chunks, factor),
        grid=(local // head_size,),
        out_shape=jax.ShapeDtypeStruct((local, total), jnp.bfloat16),
        in_specs=[spec(array) for array in (query, *keys, *values)],
        out_specs=spec(query),
        compiler_params=pltpu.CompilerParams(vmem_limit_bytes=40 * 1024 * 1024),
        cost_estimate=pl.CostEstimate(
            flops=local * total * seen * 16,
            bytes_accessed=local * (2 * total + 2 * seen) * 2,
            transcendentals=(local // head_size) * total * seen,
        ),
    )(query, *keys, *values)


def gathered(weight, axis):
    return lax.all_gather(weight, "dp", axis=axis, tiled=True)


MESH = pl.DeviceIdType.MESH
VMEM_LIMIT = 63 * 1024 * 1024
FIRST = 2
ISSUES = {0: (2,), 1: (3, 4), 2: (5,), 3: (6,), 4: (7, 8), 5: (9,), 6: (10,), 7: (11,)}
LINE_RELAYS = {5: (8,), 6: (9,), 7: (10,)}
EARLY = 4
PAIRED = (6,)
LANES = 128
NEAR = (1, 2, -1, -2)


def norm_rows(values, gain):
    wide = values.astype(jnp.float32)
    center = wide - jnp.mean(wide, axis=-1, keepdims=True)
    spread = jnp.mean(center * center, axis=-1, keepdims=True)
    return (center * lax.rsqrt(spread + 1e-06) * gain).astype(jnp.bfloat16)


def pair_dot(left, right, dims):
    return lax.dot_general(left, right, (dims, ((), ())), preferred_element_type=jnp.float32)


def remote(source, target, send, recv, device):
    return pltpu.make_async_remote_copy(
        src_ref=source, dst_ref=target, send_sem=send, recv_sem=recv,
        device_id=device, device_id_type=MESH,
    )


class Place:
    def __init__(self, line):
        self.line = line
        me, self.side = lax.axis_index("dp"), lax.axis_index("space")
        self.core, self.y, self.z = me % 2, (me // 2) % 2, me // 4
        self.sibling = {"dp": me + 1 - 2 * self.core, "space": self.side}
        self.ypeer = {"dp": me + 2 - 4 * self.y, "space": self.side}
        self.xpeer = {"dp": me, "space": 1 - self.side}

    def on_line(self, step):
        return {"dp": (self.z + step) * 4 + self.y * 2 + self.core, "space": self.side}

    def each_near(self, act):
        for step in NEAR:
            @pl.when((self.z + step >= 0) & (self.z + step < self.line))
            def _():
                act(step)

    def greet(self):
        barrier = pltpu.get_barrier_semaphore()

        def signal(device):
            pl.semaphore_signal(barrier, inc=1, device_id=device, device_id_type=MESH)

        for device in (self.sibling, self.ypeer, self.xpeer):
            signal(device)
        self.each_near(lambda step: signal(self.on_line(step)))
        before = jnp.minimum(self.z, 2)
        behind = jnp.minimum(self.line - 1 - self.z, 2)
        pl.semaphore_wait(barrier, 3 + before + behind)


class Line:
    def __init__(self, number, place, source, at, row, sems):
        self.number, self.place, self.at, self.row = number, place, at, row
        self.zsend, self.zrecv = sems[:2]
        self.mine = at(place.z, row, place.core)
        self.source = self.mine if source is None else source

    def z_copy(self, step):
        n, p = self.number, self.place
        return remote(
            self.source, self.mine, self.zsend.at[n, NEAR.index(step)], self.zrecv.at[n, p.z],
            p.on_line(step),
        )

    def z_further(self, slab, step):
        n, p = self.number, self.place
        here = self.at(slab, self.row, p.core)
        slot = 4 + slab if step > 0 else p.line + p.line - slab
        return remote(here, here, self.zsend.at[n, slot], self.zrecv.at[n, slab], p.on_line(step))

    def each_further(self, act):
        p = self.place
        for slab in range(p.line - 3):
            @pl.when((p.z - slab >= 2) & (p.z + 1 < p.line))
            def _():
                act(slab, self.z_further(slab, 1))

        for slab in range(3, p.line):
            @pl.when((slab - p.z >= 2) & (p.z >= 1))
            def _():
                act(slab, self.z_further(slab, -1))

    def passes_on(self, slab):
        p = self.place
        return ((p.z - slab >= 2) & (p.z + 1 < p.line)) | ((slab - p.z >= 2) & (p.z >= 1))

    def arrived(self, slab):
        p = self.place
        here = self.at(slab, self.row, p.core)
        remote(
            here, here, self.zsend.at[self.number, 0], self.zrecv.at[self.number, slab], p.ypeer
        ).wait_recv()

    def issue_line(self):
        self.place.each_near(lambda step: self.z_copy(step).start())

    def relay(self):
        def act(slab, copy):
            self.arrived(slab)
            copy.start()

        self.each_further(act)

    def wait_slab(self, slab):
        @pl.when((slab != self.place.z) & jnp.logical_not(self.passes_on(slab)))
        def _():
            self.arrived(slab)

    def wait_line(self):
        for slab in range(self.place.line):
            self.wait_slab(slab)

    def drain_line(self):
        self.place.each_near(lambda step: self.z_copy(step).wait_send())
        self.each_further(lambda slab, copy: copy.wait_send())


class Chunk(Line):
    def __init__(self, number, place, source, at, sems):
        super().__init__(number, place, source, at, place.y, sems)
        self.ysend, self.yrecv, self.csend, self.crecv, self.local = [
            ref.at[number] for ref in sems[2:]
        ]

    def own_copy(self):
        return pltpu.make_async_copy(self.source, self.mine, self.local)

    def y_own(self):
        return remote(self.source, self.mine, self.ysend, self.yrecv, self.place.ypeer)

    def y_part(self, slab, row):
        here = self.at(slab, row, self.place.core)
        return remote(here, here, self.ysend, self.yrecv, self.place.ypeer)

    def core_part(self, core):
        here = self.at(slice(None), slice(None), core)
        return remote(here, here, self.csend, self.crecv, self.place.sibling)

    def issue(self, over):
        self.own_copy().start()
        self.issue_line()
        if over:
            self.y_own().start()

    def forward(self):
        for slab in range(self.place.line):
            self.wait_slab(slab)

            @pl.when(slab != self.place.z)
            def _():
                self.y_part(slab, self.place.y).start()

    def mirror(self):
        self.own_copy().wait()
        self.y_part(slice(None), 1 - self.place.y).wait_recv()
        self.core_part(self.place.core).start()

    def ready(self):
        self.core_part(1 - self.place.core).wait_recv()

    def drain(self):
        self.drain_line()
        self.y_part(slice(None), self.place.y).wait_send()
        self.core_part(self.place.core).wait_send()


class PairChunk(Chunk):
    def __init__(self, number, second, place, source, at, sems):
        super().__init__(number, place, source, at, sems)
        self.second = Line(second, place, None, at, 1 - place.y, sems)

    def issue(self, over):
        self.own_copy().start()
        self.issue_line()
        self.y_part(self.place.z, 1 - self.place.y).wait_recv()
        self.second.issue_line()

    def relay(self):
        super().relay()
        self.second.relay()

    def forward(self):
        self.wait_line()
        self.second.wait_line()

    def mirror(self):
        self.own_copy().wait()
        self.core_part(self.place.core).start()

    def drain(self):
        self.drain_line()
        self.second.drain_line()
        self.y_own().wait_send()
        self.core_part(self.place.core).wait_send()


class SlabChunk:
    def __init__(self, place, source, at, send, yrecv, crecv):
        self.place, self.source, self.at = place, source, at
        self.send, self.yrecv, self.crecv = send, yrecv, crecv
        self.mine = at(place.z, place.y, place.core)

    def own_copy(self):
        return pltpu.make_async_copy(self.source, self.mine, self.send.at[2])

    def y_own(self):
        z = self.place.z
        return remote(self.source, self.mine, self.send.at[0], self.yrecv.at[z], self.place.ypeer)

    def y_copy(self, slab, row):
        here = self.at(slab, row, self.place.core)
        return remote(here, here, self.send.at[0], self.yrecv.at[slab], self.place.ypeer)

    def core_copy(self, slab, core):
        here = self.at(slab, slice(None), core)
        return remote(here, here, self.send.at[1], self.crecv.at[slab], self.place.sibling)

    def mirror(self, slab):
        @pl.when(slab == self.place.z)
        def _():
            self.own_copy().wait()

        self.y_copy(slab, 1 - self.place.y).wait_recv()
        self.core_copy(slab, self.place.core).start()

    def ready(self, slab):
        self.core_copy(slab, 1 - self.place.core).wait_recv()

    def drain(self):
        p = self.place
        whole = self.at(slice(None), p.y, p.core)
        remote(whole, whole, self.send.at[0], self.yrecv.at[0], p.ypeer).wait_send()
        whole = self.at(slice(None), slice(None), p.core)
        remote(whole, whole, self.send.at[1], self.crecv.at[0], p.sibling).wait_send()


def after_shift(values, period):
    row = lax.broadcasted_iota(jnp.int32, values.shape, 0)
    return jnp.where(row % period == 0, 0.0, pltpu.roll(values, 1, 0))


def row_chunks(total, chunk, act):
    def step(index, carry):
        act(jnp.minimum(index * chunk, total - chunk))
        return carry

    lax.fori_loop(0, -(-total // chunk), step, 0)


def keep(target, row, chunk, columns, made):
    for group in range(target.shape[0]):
        lanes = made[:, group * LANES : (group + 1) * LANES]
        target[group, pl.ds(row, chunk)] = lanes.reshape(chunk, columns, LANES)


def pick_rows(picture, field, start, count, depth):
    channels, wide = picture.shape[0], picture.shape[2]
    pairs = wide // 4
    source = lax.broadcasted_iota(jnp.int32, (wide, pairs), 0)
    pair = lax.broadcasted_iota(jnp.int32, (wide, pairs), 1)
    picks = [
        jnp.where(source == 4 * pair + phase - 1, 1.0, 0.0).astype(jnp.bfloat16)
        for phase in range(PHASES)
    ]
    pick = jnp.concatenate(picks, axis=1)
    for channel in range(channels):
        made = jnp.dot(
            picture[channel, start : start + count], pick, preferred_element_type=jnp.float32
        )
        for phase in range(PHASES):
            rows = pl.ds(start * depth + channel * PHASES + phase, count, stride=depth)
            field[rows, :] = made[:, phase * pairs : (phase + 1) * pairs]
    for spare in range(channels * PHASES, depth):
        rows = pl.ds(start * depth + spare, count, stride=depth)
        field[rows, :] = jnp.zeros((count, pairs), jnp.float32)


def two_columns(kernel, target, depth):
    taps, channels, wide = kernel.shape[0], kernel.shape[2], kernel.shape[3]
    nothing = jnp.zeros((1, wide), jnp.float32)
    target[...] = jnp.zeros_like(target)
    for tap in range(taps):
        columns = [kernel[tap, column].astype(jnp.float32) for column in range(kernel.shape[1])]
        for channel in range(channels):
            pieces = [column[channel : channel + 1] for column in columns]
            for phase in range(PHASES):
                left = pieces[phase] if phase < 3 else nothing
                right = pieces[phase - 2] if phase >= 2 else nothing
                row = tap * depth + channel * PHASES + phase
                target[row : row + 1] = jnp.concatenate([left, right], axis=1)


def conv_one(field, kernel, first, start, stop, unroll, depth, skipped):
    def step(index, carry):
        weight = kernel[...].astype(jnp.bfloat16)
        for part in range(unroll):
            row = index * unroll + part
            begin = pl.multiple_of((2 * row + skipped) * depth, depth)
            patch = field[pl.ds(begin, 3 * depth)].astype(jnp.bfloat16)
            out = pair_dot(patch, weight, ((0,), (0,)))
            first[row] = jnp.maximum(out, 0.0).astype(first.dtype)
        return carry

    lax.fori_loop(start, stop, step, 0)


def conv_two(first, kernel, second, chunk):
    total, columns = second.shape[1], first.shape[1]
    deep, wide = kernel.shape[2], kernel.shape[3]

    def act(row):
        parts, weights = [], []
        for tap in range(3):
            parts.append(jnp.concatenate([first[2 * (row + n) + tap] for n in range(chunk)], axis=0))
            before = jnp.concatenate([jnp.zeros((deep, wide), jnp.bfloat16), kernel[tap, 0]], axis=0)
            here = jnp.concatenate([kernel[tap, 1], kernel[tap, 2]], axis=0)
            weights.append(jnp.concatenate([before, here], axis=1))
        made = jnp.dot(
            jnp.concatenate(parts, axis=1), jnp.concatenate(weights, axis=0),
            preferred_element_type=jnp.float32,
        )
        out = made[:, wide:] + after_shift(made[:, :wide], columns)
        out = jnp.maximum(out, 0.0).astype(jnp.bfloat16).astype(jnp.float32)
        keep(second, row, chunk, columns, out)

    row_chunks(total, chunk, act)


def conv_later(source, kernel, chunk, row):
    columns = source.shape[2] // 2
    deep, wide = kernel.shape[2], kernel.shape[3]
    out, moved = None, None
    for tap in range(3):
        even, odd = [
            jnp.concatenate(
                [
                    jnp.concatenate(
                        [
                            source[group, 2 * (row + n) + tap, pl.ds(phase, columns, stride=2), :]
                            for n in range(chunk)
                        ],
                        axis=0,
                    )
                    for group in range(source.shape[0])
                ],
                axis=1,
            ).astype(jnp.bfloat16)
            for phase in range(2)
        ]
        here = jnp.concatenate([kernel[tap, 1], kernel[tap, 2]], axis=0)
        both = jnp.concatenate([even, odd], axis=1)
        made = jnp.dot(both, here, preferred_element_type=jnp.float32)
        late = jnp.dot(odd, kernel[tap, 0], preferred_element_type=jnp.float32)
        out = made if out is None else out + made
        moved = late if moved is None else moved + late
    return jnp.maximum(out + after_shift(moved, columns), 0.0).astype(jnp.bfloat16)


def block_body(
    line, head_size,
    images_in, kernel_one, kernel_two, kernel_three_in, kernel_four_in,
    pos_in, proj_in, gain_one, gain_two, qkv_in, out_in, up_in, down_in,
    encoded,
    picture, kernel_three, kernel_four, proj, flat, pos, tokens, normed,
    wqkv, wout, wout_other, wup, wdown, mixed, back, arrived,
    zsend, zrecv, ysend, yrecv, csend, crecv, local, down_send, down_yrecv, down_crecv, misc_send, misc_recv, misc_local,
    mix_send, mix_recv, back_send, back_recv,
):
    place = Place(line)
    side, core = place.side, place.core
    other = 1 - side
    xpeer, sibling = place.xpeer, place.sibling
    sems = (zsend, zrecv, ysend, yrecv, csend, crecv, local)
    rows, width = tokens.shape[1], tokens.shape[2]
    half = rows // 2
    count = 2 * rows
    units = up_in.shape[1]
    quarters = wup.shape[0]
    part = units // quarters
    heads = mixed.shape[1]
    margin_rows = picture.shape[1] - images_in.shape[1]
    depth = -(-images_in.shape[0] * PHASES // 16) * 16
    flat_parts = 2
    flat_rows = rows // flat_parts

    def misc(source, target, slot, device):
        return remote(source, target, misc_send.at[slot], misc_recv.at[slot], device)

    def fetch(source, target, slot):
        return pltpu.make_async_copy(source, target, misc_local.at[slot])

    own_rows = pl.ds(margin_rows, images_in.shape[1])
    own_picture = fetch(images_in, picture.at[:, own_rows], 0)
    own_picture.start()
    fetches = [
        fetch(kernel_three_in, kernel_three, 1),
        fetch(kernel_four_in, kernel_four, 2),
        fetch(proj_in, proj, 3),
        fetch(pos_in, pos.at[side], 4),
    ]
    for copy in fetches:
        copy.start()

    def at_of(ref, *lead):
        return lambda a, b, c: ref.at[(*lead, a, b, c)]

    def chunk_of(number, source, at):
        if number in PAIRED:
            second = 4 + 2 * quarters + PAIRED.index(number)
            return PairChunk(number, second, place, source, at, sems)
        return Chunk(number, place, source, at, sems)

    chunks = [chunk_of(0, out_in, at_of(wout))]
    chunks += [chunk_of(1 + n, qkv_in.at[n], at_of(wqkv, n)) for n in range(3)]
    chunks += [
        chunk_of(4 + n, up_in.at[:, pl.ds(n * part, part)], at_of(wup, n)) for n in range(quarters)
    ]
    last_chunk = len(chunks)
    down = SlabChunk(place, down_in, at_of(wdown), down_send, down_yrecv, down_crecv)
    down_parts = [
        Line(
            last_chunk + n, place, down_in.at[:, pl.ds(n * part, part)],
            lambda a, b, c, n=n: wdown.at[a, b, c, :, pl.ds(n * part, part)],
            place.y, sems,
        )
        for n in range(quarters)
    ]
    toward = jnp.where(place.z < line // 2, 1, line - 1)

    def slab_at(order):
        return (place.z + toward * order) % line

    def issue(number):
        if number < last_chunk:
            chunks[number].issue(over=number >= EARLY)
        else:
            down_parts[number - last_chunk].issue_line()

    def mirror(number):
        if number < last_chunk:
            chunks[number].mirror()
        else:
            down.mirror(slab_at(number - last_chunk))

    def relay(number):
        (chunks + down_parts)[number].relay()

    def forward(number):
        if number < last_chunk:
            chunks[number].forward()
        else:
            slab = slab_at(number - last_chunk)
            for chunk in down_parts:
                chunk.wait_slab(slab)
            down.y_copy(slab, place.y).start()

    def step(number):
        forward(number)
        if number + 1 < last_chunk:
            relay(number + 1)
        for later in LINE_RELAYS.get(number, ()):
            relay(later)
        for later in ISSUES.get(number, ()):
            issue(later)
        if number >= 1:
            mirror(number - 1)

    place.greet()
    for number in range(FIRST):
        issue(number)
    for number in (*range(EARLY), *PAIRED):
        chunks[number].y_own().start()
    down.y_own().start()
    down.own_copy().start()
    sent_margin = misc(
        images_in.at[:, pl.ds(images_in.shape[1] - margin_rows, margin_rows)],
        picture.at[:, pl.ds(0, margin_rows)], 0, xpeer,
    )

    @pl.when(side == 0)
    def _():
        sent_margin.start()

    piece = pl.ds(core * half, half)
    other_piece = pl.ds((1 - core) * half, half)
    pos_send = misc(pos_in.at[piece], pos.at[side, piece], 1, xpeer)
    pos_send.start()

    def flat_copy(where, index):
        there = pl.ds(pl.multiple_of(index * flat_rows, flat_rows), flat_rows)
        return misc(flat.at[where, there], flat.at[where, there], 5 + index, xpeer)

    def stem(field, weight_one, first, second, third):
        unroll = largest_divisor(first.shape[0], 16)
        two_columns(kernel_one, weight_one, depth)
        own_picture.wait()
        pick_rows(picture, field, margin_rows, images_in.shape[1], depth)
        relay(0)
        conv_one(field, weight_one, first, 1, first.shape[0] // unroll, unroll, depth, 1)

        @pl.when(side == 0)
        def _():
            picture[:, pl.ds(0, margin_rows)] = jnp.zeros(
                (images_in.shape[0], margin_rows, images_in.shape[2]), picture.dtype
            )

        @pl.when(side == 1)
        def _():
            sent_margin.wait_recv()

        pick_rows(picture, field, 0, margin_rows, depth)
        conv_one(field, weight_one, first, 0, 1, unroll, depth, 1)
        step(0)
        conv_two(first, kernel_two, second, 8)
        fetches[0].wait()
        chunk_three = largest_divisor(third.shape[1], 16)

        def act_three(row):
            made = conv_later(second, kernel_three, chunk_three, row)
            keep(third, row, chunk_three, third.shape[2], made.astype(jnp.float32))

        row_chunks(third.shape[1], chunk_three, act_three)
        fetches[1].wait()
        columns = third.shape[2] // 2

        def act_four(index, carry):
            made = conv_later(third, kernel_four, flat_rows // columns, index * (flat_rows // columns))
            there = pl.ds(pl.multiple_of(index * flat_rows, flat_rows), flat_rows)
            flat[side, there] = made
            flat_copy(side, index).start()
            return carry

        lax.fori_loop(0, flat_parts, act_four, 0)

    out_rows = images_in.shape[1] // 16
    counts = [(((out_rows * 2 + 1) * 2 + 1) * 2 + 1), (out_rows * 2 + 1) * 2 + 1, out_rows * 2 + 1]
    pairs = images_in.shape[2] // 4
    pl.run_scoped(
        stem,
        pltpu.VMEM((picture.shape[1] * depth, pairs), jnp.float32),
        pltpu.VMEM((3 * depth, 2 * kernel_two.shape[2]), jnp.float32),
        pltpu.VMEM((counts[0], pairs, 2 * kernel_two.shape[2]), jnp.bfloat16),
        pltpu.VMEM((kernel_two.shape[3] // LANES, counts[1], pairs, LANES), jnp.float32),
        pltpu.VMEM((kernel_three.shape[3] // LANES, counts[2], pairs // 2, LANES), jnp.float32),
    )
    step(1)
    out_cross = misc(wout.at[:, :, core], wout_other.at[:, :, core], 2, xpeer)
    out_cross.start()

    def embed(where, index):
        own = pl.ds(pl.multiple_of(index * half, half), half)
        chunk = (
            jnp.dot(flat[where, own], proj[...], preferred_element_type=jnp.float32)
            + pos[where, own].astype(jnp.float32)
        ).astype(jnp.bfloat16)
        tokens[where, own] = chunk
        normed[where, own] = norm_rows(chunk, gain_one[...])

    fetches[2].wait()
    fetches[3].wait()
    embed(side, 0)
    embed(side, 1)
    arriving = pos.at[other, piece]
    misc(arriving, arriving, 1, xpeer).wait_recv()
    pos_mirror = misc(arriving, arriving, 3, sibling)
    pos_mirror.start()
    step(2)
    coming = pos.at[other, other_piece]
    misc(coming, coming, 3, sibling).wait_recv()
    for index in range(flat_parts):
        flat_copy(other, index).wait_recv()
    embed(other, 0)
    embed(other, 1)
    step(3)
    step(4)
    cross = wout_other.at[:, :, core]
    misc(cross, cross, 2, xpeer).wait_recv()
    out_mirror = misc(cross, cross, 4, sibling)
    out_mirror.start()

    def attention(qkv):
        for n in range(3):
            chunks[1 + n].ready()

        def project(index, carry):
            which, where = index // 2, index % 2
            weight = wqkv[which].reshape(width, heads * head_size)
            made = pair_dot(weight, normed[where], ((0,), (1,)))
            columns = pl.ds(pl.multiple_of(where * rows, rows), rows)
            qkv[which, :, :, columns] = made.astype(jnp.bfloat16).reshape(heads, head_size, rows)
            return carry

        lax.fori_loop(0, 6, project, 0)
        factor = math.log2(math.e) / math.sqrt(head_size)
        block = largest_divisor(count // 128, 2) * 128

        def attend_head(head, carry):
            keys, values = qkv[1, head], qkv[2, head]
            for start in range(0, count, block):
                query = qkv[0, head, :, start : start + block]
                score = pair_dot(keys, query, ((0,), (0,)))
                top = jnp.max(score, axis=0, keepdims=True)
                weight = jnp.exp2((score - top) * factor)
                below = jnp.sum(weight, axis=0, keepdims=True)
                made = jnp.dot(values, weight.astype(jnp.bfloat16), preferred_element_type=jnp.float32)
                mixed[side, head, :, start : start + block] = (made / below).astype(jnp.bfloat16)
            mix_copy(side, head).start()
            for number, when in ((5, heads // 8), (6, heads * 4 // 8), (7, heads * 7 // 8)):
                @pl.when(head == when)
                def _():
                    step(number)

            return carry

        lax.fori_loop(0, heads, attend_head, 0)

    def mix_copy(where, head):
        return remote(mixed.at[where, head], mixed.at[where, head], mix_send.at[head], mix_recv.at[head], xpeer)

    pl.run_scoped(attention, pltpu.VMEM((3, heads, head_size, count), jnp.bfloat16))
    relay(last_chunk + quarters - 1)
    chunks[0].ready()
    cross_other = wout_other.at[:, :, 1 - core]
    misc(cross_other, cross_other, 4, sibling).wait_recv()
    for head in range(heads):
        mix_copy(other, head).wait_recv()

    def settle(index, carry):
        where, first = index // 2, pl.multiple_of((index % 2) * half, half)
        columns = pl.ds(pl.multiple_of(index * half, half), half)
        own = pl.ds(first, half)
        attn = tokens[where, own].astype(jnp.float32)
        for share_of, weight in ((side, wout), (other, wout_other)):
            left = mixed[share_of, :, :, columns].reshape(heads * head_size, half)
            share = pair_dot(left, weight[...].reshape(width, heads * head_size), ((0,), (1,)))
            attn = attn + share.astype(jnp.bfloat16).astype(jnp.float32)
        chunk = attn.astype(jnp.bfloat16)
        tokens[where, own] = chunk
        normed[where, own] = norm_rows(chunk, gain_two[...])
        return carry

    lax.fori_loop(0, 2, settle, 0)
    mirror(last_chunk - 1)
    step(last_chunk + 1)
    lax.fori_loop(2, 4, settle, 0)
    slab_rows = width // line

    def back_copy(slab):
        there = pl.ds(pl.multiple_of(slab * slab_rows, slab_rows), slab_rows)
        return remote(back.at[there], arrived.at[there], back_send.at[slab], back_recv.at[slab], xpeer)

    def feed(hidden, total):
        for quarter in range(quarters):
            chunks[4 + quarter].ready()

            def rise(where, carry):
                weight = wup[quarter].reshape(width, part)
                before = jnp.dot(normed[where], weight, preferred_element_type=jnp.float32)
                made = 0.5 * before * (1.0 + lax.erf(before * math.sqrt(0.5)))
                hidden[where, :, quarter * part : (quarter + 1) * part] = made.astype(jnp.bfloat16)
                return carry

            lax.fori_loop(0, 2, rise, 0)
            if quarter == 1:
                step(10)

        def fall(order):
            slab = slab_at(order)
            down.ready(slab)
            there = pl.ds(pl.multiple_of(slab * slab_rows, slab_rows), slab_rows)
            weight = wdown[slab].reshape(slab_rows, units)
            back[there] = pair_dot(weight, hidden[other], ((1,), (1,))).astype(jnp.bfloat16)
            back_copy(slab).start()
            total[there] = pair_dot(weight, hidden[side], ((1,), (1,))).astype(jnp.bfloat16)

        fall(0)
        for order in range(3, line):
            step(last_chunk + order)
        for order in range(1, line):
            if order == line - 1:
                mirror(last_chunk + order)
            fall(order)
        for slab in range(line):
            back_copy(slab).wait_recv()
        summed = total[...].astype(jnp.float32) + arrived[...].astype(jnp.float32)
        encoded[...] = (tokens[side].astype(jnp.float32) + summed.T).astype(jnp.bfloat16)

    pl.run_scoped(
        feed, pltpu.VMEM((2, rows, units), jnp.bfloat16), pltpu.VMEM((width, rows), jnp.bfloat16)
    )

    @pl.when(side == 0)
    def _():
        sent_margin.wait_send()

    for copy in (pos_send, out_cross, pos_mirror, out_mirror):
        copy.wait_send()
    for index in range(flat_parts):
        flat_copy(side, index).wait_send()
    for head in range(heads):
        mix_copy(side, head).wait_send()
    for slab in range(line):
        back_copy(slab).wait_send()
    for chunk in chunks:
        chunk.drain()
    for chunk in down_parts:
        chunk.drain_line()
    down.drain()


def whole_block(
    images, pos, kernel_one, kernel_two, kernel_three, kernel_four, proj, gain_one, gain_two,
    qkv_shard, out_shard, up_shard, down_shard,
):
    line = lax.axis_size("dp") // 4
    depth, local, units = qkv_shard.shape[1], qkv_shard.shape[2], up_shard.shape[1]
    rows, width = pos.shape
    head_size = width // HEADS
    heads = local // head_size
    quarters = 4
    numbers = 4 + 2 * quarters + len(PAIRED)
    whole = 4 + quarters
    here = (line, 2, 2, depth)
    bf16 = jnp.bfloat16
    vmem = pl.BlockSpec(memory_space=pltpu.VMEM)
    hbm = pl.BlockSpec(memory_space=pl.ANY)
    dma = pltpu.SemaphoreType.DMA
    return pl.pallas_call(
        functools.partial(block_body, line, head_size),
        out_shape=jax.ShapeDtypeStruct((rows, width), bf16),
        in_specs=[hbm, vmem, vmem, hbm, hbm, hbm, hbm, vmem, vmem, hbm, hbm, hbm, hbm],
        out_specs=vmem,
        scratch_shapes=[
            pltpu.VMEM((images.shape[1], images.shape[2] + 16, images.shape[3]), bf16),
            pltpu.VMEM(kernel_three.shape, bf16),
            pltpu.VMEM(kernel_four.shape, bf16),
            pltpu.VMEM(proj.shape, bf16),
            pltpu.VMEM((2, rows, proj.shape[0]), bf16),
            pltpu.VMEM((2, rows, width), bf16),
            pltpu.VMEM((2, rows, width), bf16),
            pltpu.VMEM((2, rows, width), bf16),
            pltpu.VMEM((3, *here, local), bf16),
            pltpu.VMEM((*here, local), bf16),
            pltpu.VMEM((*here, local), bf16),
            pltpu.VMEM((quarters, *here, units // quarters), bf16),
            pltpu.VMEM((*here, units), bf16),
            pltpu.VMEM((2, heads, head_size, 2 * rows), bf16),
            pltpu.VMEM((width, rows), bf16),
            pltpu.VMEM((width, rows), bf16),
            dma((numbers, 4 + 2 * (line - 3))),
            dma((numbers, line)),
            dma((whole,)),
            dma((whole,)),
            dma((whole,)),
            dma((whole,)),
            dma((whole,)),
            dma((3,)),
            dma((line,)),
            dma((line,)),
            dma((7,)),
            dma((7,)),
            dma((5,)),
            dma((heads,)),
            dma((heads,)),
            dma((line,)),
            dma((line,)),
        ],
        compiler_params=pltpu.CompilerParams(
            collective_id=0, has_side_effects=True, vmem_limit_bytes=VMEM_LIMIT
        ),
    )(
        images[0], kernel_one, kernel_two, kernel_three, kernel_four, pos, proj, gain_one, gain_two,
        qkv_shard, out_shard, up_shard, down_shard,
    )


def on_ring(
    images,
    pos_embed,
    conv_first,
    conv_second,
    conv_third,
    conv_fourth,
    proj_weight,
    ln_first,
    qkv_weight,
    out_weight,
    ln_second,
    up_weight,
    down_weight,
):
    count = lax.axis_size("space")
    attention_part = gathered(
        jnp.concatenate([jnp.moveaxis(qkv_weight, 1, 0), out_weight.T[None]], axis=0), 1
    )
    feed_part = gathered(jnp.stack([up_weight, down_weight.T]), 1)
    out_part = attention_part[3]
    up_part, down_part = feed_part[0], feed_part[1]
    margin = passed_along(images[:, :, -15:, :], "space", 1)
    positions = [pos_embed] + [shifted(pos_embed, "space", k) for k in range(1, count)]

    stem_out = second_conv(first_conv(images, margin, conv_first), conv_second)
    for kernel in (conv_third, conv_fourth):
        stem_out = later_conv(stem_out, kernel)
    flat = stem_out.reshape(-1, stem_out.shape[3])
    flats = [flat] + [shifted(flat, "space", k) for k in range(1, count)]
    width = proj_weight.shape[1]
    local = attention_part.shape[2]
    head_size = width // HEADS

    tokens = None
    projected = []
    for rows, position in zip(flats, positions):
        chunk = (
            jnp.dot(rows, proj_weight, preferred_element_type=jnp.float32)
            + position.astype(jnp.float32)
        ).astype(jnp.bfloat16)
        tokens = chunk if tokens is None else tokens
        normed = layer_norm(chunk, ln_first)
        projected.append(
            [
                lax.dot_general(
                    attention_part[which],
                    normed,
                    (((0,), (1,)), ((), ())),
                    preferred_element_type=jnp.float32,
                ).astype(jnp.bfloat16)
                for which in range(3)
            ]
        )
    keys = [part[1] for part in projected]
    values = [part[2] for part in projected]

    def attention_share(query):
        mixed = attend(query, keys, values, head_size)
        share = lax.dot_general(
            mixed, out_part, (((0,), (1,)), ((), ())), preferred_element_type=jnp.float32
        ).astype(jnp.bfloat16)
        return mixed, share

    returned = []
    last = None
    for k in list(range(1, count)) + [0]:
        query = projected[k][0]
        if last is not None:
            query, _ = lax.optimization_barrier((query, last))
        last, share = attention_share(query)
        returned.append(shifted(share, "space", -k) if k else share)
    attn_sum = sum(part.astype(jnp.float32) for part in returned)
    after_attn = (tokens.astype(jnp.float32) + attn_sum).astype(jnp.bfloat16)
    normed_two = layer_norm(after_attn, ln_second)

    def feed_forward(rows):
        before = jnp.dot(rows, up_part, preferred_element_type=jnp.float32)
        hidden = (0.5 * before * (1.0 + lax.erf(before * math.sqrt(0.5)))).astype(jnp.bfloat16)
        hidden = lax.optimization_barrier(hidden)
        return lax.dot_general(
            hidden, down_part, (((1,), (1,)), ((), ())), preferred_element_type=jnp.float32
        ).astype(jnp.bfloat16)

    rows = normed_two.shape[0]
    half = rows // 2
    pieces = [normed_two[:half], normed_two[half:]]
    moved = [[shifted(piece, "space", k) for piece in pieces] for k in range(1, count)]
    totals = feed_forward(normed_two).astype(jnp.float32)
    back = [
        jnp.concatenate([shifted(feed_forward(piece), "space", -k) for piece in there], axis=0)
        for k, there in zip(range(1, count), moved)
    ]
    for part in back:
        totals = totals + part.astype(jnp.float32)
    return (after_attn.astype(jnp.float32) + totals).astype(jnp.bfloat16)[None]


def on_device(
    images,
    pos_embed,
    conv_first,
    conv_second,
    conv_third,
    conv_fourth,
    proj_weight,
    ln_first,
    qkv_weight,
    out_weight,
    ln_second,
    up_weight,
    down_weight,
):
    shards = lax.axis_size("dp")
    fits = lax.axis_size("space") == 2 and shards % 16 == 0 and images.shape[0] == 1
    fits = fits and qkv_weight.shape[0] % 16 == 0 and qkv_weight.shape[2] % 128 == 0
    if not fits:
        return on_ring(
            images, pos_embed, conv_first, conv_second, conv_third, conv_fourth, proj_weight,
            ln_first, qkv_weight, out_weight, ln_second, up_weight, down_weight,
        )
    out = whole_block(
        images, pos_embed, conv_first, conv_second, conv_third, conv_fourth, proj_weight,
        ln_first, ln_second,
        jnp.moveaxis(qkv_weight, 1, 0), out_weight.T, up_weight, down_weight.T,
    )
    return out[None]


def solution(mesh):
    placed = (
        P("dp", None, "space", None),
        P("space", None),
        P(),
        P(),
        P(),
        P(),
        P(),
        P(),
        P("dp", None, "space"),
        P("space", "dp"),
        P(),
        P("dp", "space"),
        P("space", "dp"),
    )
    return jax.shard_map(
        on_device, mesh=mesh, in_specs=placed, out_specs=P("dp", "space", None), check_vma=False
    )
```

```python
import functools
import math

import jax
import jax.numpy as jnp
from jax import lax
from jax.experimental import pallas as pl
from jax.experimental.pallas import tpu as pltpu
from jax.sharding import PartitionSpec as P

HEADS = 16
PHASES = 5


def passed_along(value, axis, steps):
    count = lax.axis_size(axis)
    leading, last = (max(0, -steps), min(count, count - steps))
    return lax.ppermute(value, axis, [(source, source + steps) for source in range(leading, last)])


def shifted(value, axis, steps):
    count = lax.axis_size(axis)
    return lax.ppermute(value, axis, [(source, (source + steps) % count) for source in range(count)])


def largest_divisor(number, limit):
    return max(d for d in range(1, limit + 1) if number % d == 0)


def first_conv_body(unroll, field_ref, kernel_ref, out_ref):
    depth = field_ref.shape[1]
    lanes = field_ref.shape[2]

    def step(index, carry):
        for part in range(unroll):
            row = index * unroll + part
            patch = field_ref[pl.ds(2 * row, 3)].reshape(3 * depth, lanes)
            out = lax.dot_general(
                patch, kernel_ref[...], (((0,), (0,)), ((), ())), preferred_element_type=jnp.float32
            )
            out_ref[row] = jnp.maximum(out, 0.0).astype(out_ref.dtype)
        return carry

    lax.fori_loop(0, out_ref.shape[0] // unroll, step, 0)


def first_conv(images, margin, kernel):
    wide = images.shape[3]
    pairs = wide // 4
    channels = images.shape[1]
    out_channels = kernel.shape[3]
    source = lax.broadcasted_iota(jnp.int32, (wide, PHASES, pairs), 0)
    phase = lax.broadcasted_iota(jnp.int32, (wide, PHASES, pairs), 1)
    pair = lax.broadcasted_iota(jnp.int32, (wide, PHASES, pairs), 2)
    pick = (source == 4 * pair + phase - 1).astype(jnp.bfloat16)
    field = jnp.concatenate([margin, images], axis=2)[0]
    rows = field.shape[1]
    picked = jnp.einsum("chw,wqp->hcqp", field, pick, preferred_element_type=jnp.float32)
    picked = picked.astype(jnp.bfloat16).reshape(rows, channels * PHASES, pairs)
    depth = -(-channels * PHASES // 16) * 16
    picked = jnp.pad(picked, ((0, 0), (0, depth - channels * PHASES), (0, 0)))
    taps = jnp.transpose(kernel, (0, 2, 1, 3))
    left = jnp.pad(taps, ((0, 0), (0, 0), (0, 2), (0, 0)))
    right = jnp.pad(taps, ((0, 0), (0, 0), (2, 0), (0, 0)))
    both = jnp.concatenate([left, right], axis=3).reshape(3, channels * PHASES, 2 * out_channels)
    both = jnp.pad(both, ((0, 0), (0, depth - channels * PHASES), (0, 0)))
    both = both.reshape(3 * depth, 2 * out_channels)
    count = (rows - 3) // 2 + 1
    out = pl.pallas_call(
        functools.partial(first_conv_body, largest_divisor(count, 16)),
        out_shape=jax.ShapeDtypeStruct((count, pairs, 2 * out_channels), jnp.bfloat16),
        in_specs=[pl.BlockSpec(memory_space=pltpu.VMEM)] * 2,
        out_specs=pl.BlockSpec(memory_space=pltpu.VMEM),
        compiler_params=pltpu.CompilerParams(vmem_limit_bytes=40 * 1024 * 1024),
        cost_estimate=pl.CostEstimate(
            flops=count * pairs * depth * 3 * 4 * out_channels * 4,
            bytes_accessed=count * pairs * out_channels * 4,
            transcendentals=0,
        ),
    )(picked, both)
    return out[None]


def second_conv(field, kernel):
    height, _, inner, outer = kernel.shape
    before = jnp.concatenate([jnp.zeros_like(kernel[:, 0]), kernel[:, 0]], axis=1)
    here = jnp.concatenate([kernel[:, 1], kernel[:, 2]], axis=1)
    paired = jnp.stack([before, here], axis=1)
    out = lax.conv_general_dilated(
        field,
        paired,
        (2, 1),
        ((0, 0), (1, 0)),
        dimension_numbers=("NHWC", "HWIO", "NHWC"),
        preferred_element_type=jnp.float32,
    )
    return jax.nn.relu(out).astype(jnp.bfloat16)


def later_conv(field, kernel):
    out = lax.conv_general_dilated(
        field,
        kernel,
        (2, 2),
        ((0, 0), (1, 1)),
        dimension_numbers=("NHWC", "HWIO", "NHWC"),
        preferred_element_type=jnp.float32,
    )
    return jax.nn.relu(out).astype(jnp.bfloat16)


def layer_norm(values, gain):
    wide = values.astype(jnp.float32)
    center = wide - jnp.mean(wide, axis=-1, keepdims=True)
    spread = jnp.mean(center * center, axis=-1, keepdims=True)
    return (center * lax.rsqrt(spread + 1e-06) * gain).astype(jnp.bfloat16)


def attend_body(chunks, factor, *refs):
    query_ref, out_ref = refs[0], refs[-1]
    keys, values = refs[1 : 1 + chunks], refs[1 + chunks : 1 + 2 * chunks]
    total = query_ref.shape[1]
    block = largest_divisor(total // 128, 2) * 128
    for start in range(0, total, block):
        query = query_ref[:, start : start + block]
        scores = [
            lax.dot_general(
                key[...], query, (((0,), (0,)), ((), ())), preferred_element_type=jnp.float32
            )
            for key in keys
        ]
        top = functools.reduce(
            jnp.maximum, [jnp.max(score, axis=0, keepdims=True) for score in scores]
        )
        weights = [jnp.exp2((score - top) * factor) for score in scores]
        below = sum(jnp.sum(weight, axis=0, keepdims=True) for weight in weights)
        mixed = sum(
            jnp.dot(value[...], weight.astype(jnp.bfloat16), preferred_element_type=jnp.float32)
            for value, weight in zip(values, weights)
        )
        out_ref[:, start : start + block] = (mixed / below).astype(out_ref.dtype)


def attend(query, keys, values, head_size):
    local, total = query.shape
    chunks = len(keys)
    seen = sum(key.shape[1] for key in keys)
    spec = lambda array: pl.BlockSpec((head_size, array.shape[1]), lambda head: (head, 0))
    factor = math.log2(math.e) / math.sqrt(head_size)
    return pl.pallas_call(
        functools.partial(attend_body, chunks, factor),
        grid=(local // head_size,),
        out_shape=jax.ShapeDtypeStruct((local, total), jnp.bfloat16),
        in_specs=[spec(array) for array in (query, *keys, *values)],
        out_specs=spec(query),
        compiler_params=pltpu.CompilerParams(vmem_limit_bytes=40 * 1024 * 1024),
        cost_estimate=pl.CostEstimate(
            flops=local * total * seen * 16,
            bytes_accessed=local * (2 * total + 2 * seen) * 2,
            transcendentals=(local // head_size) * total * seen,
        ),
    )(query, *keys, *values)


def gathered(weight, axis):
    return lax.all_gather(weight, "dp", axis=axis, tiled=True)


MESH = pl.DeviceIdType.MESH
VMEM_LIMIT = 63 * 1024 * 1024
FIRST = 2
ISSUES = {0: (2,), 1: (3, 4), 2: (5,), 3: (6,), 4: (7,)}
EARLY = 6
PLACED = ((5, 1), (6, 5), (7, 10))
PAIRED = ()
LANES = 128
NEAR = (1, 2, -1, -2)


def norm_rows(values, gain):
    wide = values.astype(jnp.float32)
    center = wide - jnp.mean(wide, axis=-1, keepdims=True)
    spread = jnp.mean(center * center, axis=-1, keepdims=True)
    return (center * lax.rsqrt(spread + 1e-06) * gain).astype(jnp.bfloat16)


def pair_dot(left, right, dims):
    return lax.dot_general(left, right, (dims, ((), ())), preferred_element_type=jnp.float32)


def remote(source, target, send, recv, device):
    return pltpu.make_async_remote_copy(
        src_ref=source, dst_ref=target, send_sem=send, recv_sem=recv,
        device_id=device, device_id_type=MESH,
    )


class Place:
    def __init__(self, line):
        self.line = line
        me, self.side = lax.axis_index("dp"), lax.axis_index("space")
        self.core, self.y, self.z = me % 2, (me // 2) % 2, me // 4
        self.sibling = {"dp": me + 1 - 2 * self.core, "space": self.side}
        self.ypeer = {"dp": me + 2 - 4 * self.y, "space": self.side}
        self.xpeer = {"dp": me, "space": 1 - self.side}

    def on_line(self, step):
        return {"dp": (self.z + step) * 4 + self.y * 2 + self.core, "space": self.side}

    def each_near(self, act, steps=NEAR):
        for step in steps:
            @pl.when((self.z + step >= 0) & (self.z + step < self.line))
            def _():
                act(step)

    def greet(self):
        barrier = pltpu.get_barrier_semaphore()

        def signal(device):
            pl.semaphore_signal(barrier, inc=1, device_id=device, device_id_type=MESH)

        for device in (self.sibling, self.ypeer, self.xpeer):
            signal(device)
        self.each_near(lambda step: signal(self.on_line(step)))
        before = jnp.minimum(self.z, 2)
        behind = jnp.minimum(self.line - 1 - self.z, 2)
        pl.semaphore_wait(barrier, 3 + before + behind)


class Line:
    def __init__(self, number, place, source, at, row, sems):
        self.number, self.place, self.at, self.row = number, place, at, row
        self.zsend, self.zrecv = sems[:2]
        self.mine = at(place.z, row, place.core)
        self.source = self.mine if source is None else source

    def z_copy(self, step):
        n, p = self.number, self.place
        return remote(
            self.source, self.mine, self.zsend.at[n, NEAR.index(step)], self.zrecv.at[n, p.z],
            p.on_line(step),
        )

    def z_further(self, slab, step):
        n, p = self.number, self.place
        here = self.at(slab, self.row, p.core)
        slot = 4 + slab if step > 0 else p.line + p.line - slab
        return remote(here, here, self.zsend.at[n, slot], self.zrecv.at[n, slab], p.on_line(step))

    def each_further(self, act):
        p = self.place
        for slab in range(p.line - 3):
            @pl.when((p.z - slab >= 2) & (p.z + 1 < p.line))
            def _():
                act(slab, self.z_further(slab, 1))

        for slab in range(3, p.line):
            @pl.when((slab - p.z >= 2) & (p.z >= 1))
            def _():
                act(slab, self.z_further(slab, -1))

    def passes_on(self, slab):
        p = self.place
        return ((p.z - slab >= 2) & (p.z + 1 < p.line)) | ((slab - p.z >= 2) & (p.z >= 1))

    def arrived(self, slab):
        p = self.place
        here = self.at(slab, self.row, p.core)
        remote(
            here, here, self.zsend.at[self.number, 0], self.zrecv.at[self.number, slab], p.ypeer
        ).wait_recv()

    def issue_line(self, steps=NEAR):
        self.place.each_near(lambda step: self.z_copy(step).start(), steps)

    def relay(self):
        def act(slab, copy):
            self.arrived(slab)
            copy.start()

        self.each_further(act)

    def wait_slab(self, slab):
        @pl.when((slab != self.place.z) & jnp.logical_not(self.passes_on(slab)))
        def _():
            self.arrived(slab)

    def wait_line(self):
        for slab in range(self.place.line):
            self.wait_slab(slab)

    def drain_line(self):
        self.place.each_near(lambda step: self.z_copy(step).wait_send())
        self.each_further(lambda slab, copy: copy.wait_send())


class Chunk(Line):
    def __init__(self, number, place, source, at, sems):
        super().__init__(number, place, source, at, place.y, sems)
        self.ysend, self.yrecv, self.csend, self.crecv, self.local = [
            ref.at[number] for ref in sems[2:]
        ]

    def own_copy(self):
        return pltpu.make_async_copy(self.source, self.mine, self.local)

    def y_own(self):
        return remote(self.source, self.mine, self.ysend, self.yrecv, self.place.ypeer)

    def y_part(self, slab, row):
        here = self.at(slab, row, self.place.core)
        return remote(here, here, self.ysend, self.yrecv, self.place.ypeer)

    def core_part(self, core):
        here = self.at(slice(None), slice(None), core)
        return remote(here, here, self.csend, self.crecv, self.place.sibling)

    def issue(self, over):
        self.own_copy().start()
        self.issue_line()
        if over:
            self.y_own().start()

    def forward(self):
        for slab in range(self.place.line):
            self.wait_slab(slab)

            @pl.when(slab != self.place.z)
            def _():
                self.y_part(slab, self.place.y).start()

    def mirror(self):
        self.own_copy().wait()
        self.y_part(slice(None), 1 - self.place.y).wait_recv()
        self.core_part(self.place.core).start()

    def ready(self):
        self.core_part(1 - self.place.core).wait_recv()

    def drain(self):
        self.drain_line()
        self.y_part(slice(None), self.place.y).wait_send()
        self.core_part(self.place.core).wait_send()


class PairChunk(Chunk):
    def __init__(self, number, second, place, source, at, sems):
        super().__init__(number, place, source, at, sems)
        self.second = Line(second, place, None, at, 1 - place.y, sems)

    def issue(self, over):
        self.own_copy().start()
        self.issue_line()
        self.y_part(self.place.z, 1 - self.place.y).wait_recv()
        self.second.issue_line()

    def relay(self):
        super().relay()
        self.second.relay()

    def forward(self):
        self.wait_line()
        self.second.wait_line()

    def mirror(self):
        self.own_copy().wait()
        self.core_part(self.place.core).start()

    def drain(self):
        self.drain_line()
        self.second.drain_line()
        self.y_own().wait_send()
        self.core_part(self.place.core).wait_send()


class SlabChunk:
    def __init__(self, place, source, at, send, yrecv, crecv):
        self.place, self.source, self.at = place, source, at
        self.send, self.yrecv, self.crecv = send, yrecv, crecv
        self.mine = at(place.z, place.y, place.core)

    def own_copy(self):
        return pltpu.make_async_copy(self.source, self.mine, self.send.at[2])

    def y_own(self):
        z = self.place.z
        return remote(self.source, self.mine, self.send.at[0], self.yrecv.at[z], self.place.ypeer)

    def y_copy(self, slab, row):
        here = self.at(slab, row, self.place.core)
        return remote(here, here, self.send.at[0], self.yrecv.at[slab], self.place.ypeer)

    def core_copy(self, slab, core):
        here = self.at(slab, slice(None), core)
        return remote(here, here, self.send.at[1], self.crecv.at[slab], self.place.sibling)

    def mirror(self, slab):
        @pl.when(slab == self.place.z)
        def _():
            self.own_copy().wait()

        self.y_copy(slab, 1 - self.place.y).wait_recv()
        self.core_copy(slab, self.place.core).start()

    def ready(self, slab):
        self.core_copy(slab, 1 - self.place.core).wait_recv()

    def drain(self):
        p = self.place
        whole = self.at(slice(None), p.y, p.core)
        remote(whole, whole, self.send.at[0], self.yrecv.at[0], p.ypeer).wait_send()
        whole = self.at(slice(None), slice(None), p.core)
        remote(whole, whole, self.send.at[1], self.crecv.at[0], p.sibling).wait_send()


def after_shift(values, period):
    row = lax.broadcasted_iota(jnp.int32, values.shape, 0)
    return jnp.where(row % period == 0, 0.0, pltpu.roll(values, 1, 0))


def row_chunks(total, chunk, act):
    def step(index, carry):
        act(jnp.minimum(index * chunk, total - chunk))
        return carry

    lax.fori_loop(0, -(-total // chunk), step, 0)


def keep(target, row, chunk, columns, made):
    for group in range(target.shape[0]):
        lanes = made[:, group * LANES : (group + 1) * LANES]
        target[group, pl.ds(row, chunk)] = lanes.reshape(chunk, columns, LANES)


def pick_rows(picture, field, start, count, depth):
    channels, wide = picture.shape[0], picture.shape[2]
    pairs = wide // 4
    source = lax.broadcasted_iota(jnp.int32, (wide, pairs), 0)
    pair = lax.broadcasted_iota(jnp.int32, (wide, pairs), 1)
    picks = [
        jnp.where(source == 4 * pair + phase - 1, 1.0, 0.0).astype(jnp.bfloat16)
        for phase in range(PHASES)
    ]
    pick = jnp.concatenate(picks, axis=1)
    for channel in range(channels):
        made = jnp.dot(
            picture[channel, start : start + count], pick, preferred_element_type=jnp.float32
        )
        for phase in range(PHASES):
            rows = pl.ds(start * depth + channel * PHASES + phase, count, stride=depth)
            field[rows, :] = made[:, phase * pairs : (phase + 1) * pairs]
    for spare in range(channels * PHASES, depth):
        rows = pl.ds(start * depth + spare, count, stride=depth)
        field[rows, :] = jnp.zeros((count, pairs), jnp.float32)


def two_columns(kernel, target, depth):
    taps, channels, wide = kernel.shape[0], kernel.shape[2], kernel.shape[3]
    nothing = jnp.zeros((1, wide), jnp.float32)
    target[...] = jnp.zeros_like(target)
    for tap in range(taps):
        columns = [kernel[tap, column].astype(jnp.float32) for column in range(kernel.shape[1])]
        for channel in range(channels):
            pieces = [column[channel : channel + 1] for column in columns]
            for phase in range(PHASES):
                left = pieces[phase] if phase < 3 else nothing
                right = pieces[phase - 2] if phase >= 2 else nothing
                row = tap * depth + channel * PHASES + phase
                target[row : row + 1] = jnp.concatenate([left, right], axis=1)


def conv_one(field, kernel, first, start, stop, unroll, depth, skipped):
    def step(index, carry):
        weight = kernel[...].astype(jnp.bfloat16)
        for part in range(unroll):
            row = index * unroll + part
            begin = pl.multiple_of((2 * row + skipped) * depth, depth)
            patch = field[pl.ds(begin, 3 * depth)].astype(jnp.bfloat16)
            out = pair_dot(patch, weight, ((0,), (0,)))
            first[row] = jnp.maximum(out, 0.0).astype(first.dtype)
        return carry

    lax.fori_loop(start, stop, step, 0)


def conv_two(first, kernel, second, chunk):
    total, columns = second.shape[1], first.shape[1]
    deep, wide = kernel.shape[2], kernel.shape[3]

    def act(row):
        parts, weights = [], []
        for tap in range(3):
            parts.append(jnp.concatenate([first[2 * (row + n) + tap] for n in range(chunk)], axis=0))
            before = jnp.concatenate([jnp.zeros((deep, wide), jnp.bfloat16), kernel[tap, 0]], axis=0)
            here = jnp.concatenate([kernel[tap, 1], kernel[tap, 2]], axis=0)
            weights.append(jnp.concatenate([before, here], axis=1))
        made = jnp.dot(
            jnp.concatenate(parts, axis=1), jnp.concatenate(weights, axis=0),
            preferred_element_type=jnp.float32,
        )
        out = made[:, wide:] + after_shift(made[:, :wide], columns)
        out = jnp.maximum(out, 0.0).astype(jnp.bfloat16).astype(jnp.float32)
        keep(second, row, chunk, columns, out)

    row_chunks(total, chunk, act)


def conv_later(source, kernel, chunk, row):
    columns = source.shape[2] // 2
    deep, wide = kernel.shape[2], kernel.shape[3]
    out, moved = None, None
    for tap in range(3):
        even, odd = [
            jnp.concatenate(
                [
                    jnp.concatenate(
                        [
                            source[group, 2 * (row + n) + tap, pl.ds(phase, columns, stride=2), :]
                            for n in range(chunk)
                        ],
                        axis=0,
                    )
                    for group in range(source.shape[0])
                ],
                axis=1,
            ).astype(jnp.bfloat16)
            for phase in range(2)
        ]
        here = jnp.concatenate([kernel[tap, 1], kernel[tap, 2]], axis=0)
        both = jnp.concatenate([even, odd], axis=1)
        made = jnp.dot(both, here, preferred_element_type=jnp.float32)
        late = jnp.dot(odd, kernel[tap, 0], preferred_element_type=jnp.float32)
        out = made if out is None else out + made
        moved = late if moved is None else moved + late
    return jnp.maximum(out + after_shift(moved, columns), 0.0).astype(jnp.bfloat16)


def block_body(
    line, head_size,
    images_in, kernel_one, kernel_two, kernel_three_in, kernel_four_in,
    pos_in, proj_in, gain_one, gain_two, qkv_in, out_in, up_in, down_in,
    encoded,
    picture, kernel_three, kernel_four, proj, flat, pos, tokens, normed,
    wqkv, wout, wout_other, wup, wdown, mixed, back, arrived,
    zsend, zrecv, ysend, yrecv, csend, crecv, local, down_send, down_yrecv, down_crecv, misc_send, misc_recv, misc_local,
    mix_send, mix_recv, back_send, back_recv,
):
    place = Place(line)
    side, core = place.side, place.core
    other = 1 - side
    xpeer, sibling = place.xpeer, place.sibling
    sems = (zsend, zrecv, ysend, yrecv, csend, crecv, local)
    rows, width = tokens.shape[1], tokens.shape[2]
    half = rows // 2
    count = 2 * rows
    units = up_in.shape[1]
    quarters = wup.shape[0]
    part = units // quarters
    heads = mixed.shape[2]
    margin_rows = picture.shape[1] - images_in.shape[1]
    depth = -(-images_in.shape[0] * PHASES // 16) * 16
    flat_parts = 2
    flat_rows = rows // flat_parts

    def misc(source, target, slot, device):
        return remote(source, target, misc_send.at[slot], misc_recv.at[slot], device)

    def fetch(source, target, slot):
        return pltpu.make_async_copy(source, target, misc_local.at[slot])

    own_rows = pl.ds(margin_rows, images_in.shape[1])
    own_picture = fetch(images_in, picture.at[:, own_rows], 0)
    own_picture.start()
    fetches = [
        fetch(kernel_three_in, kernel_three, 1),
        fetch(kernel_four_in, kernel_four, 2),
        fetch(proj_in, proj, 3),
        fetch(pos_in, pos.at[side], 4),
    ]
    for copy in fetches:
        copy.start()

    def at_of(ref, *lead):
        return lambda a, b, c: ref.at[(*lead, a, b, c)]

    def chunk_of(number, source, at):
        if number in PAIRED:
            second = 5 + quarters + PAIRED.index(number)
            return PairChunk(number, second, place, source, at, sems)
        return Chunk(number, place, source, at, sems)

    chunks = [chunk_of(0, out_in, at_of(wout))]
    chunks += [chunk_of(1 + n, qkv_in.at[n], at_of(wqkv, n)) for n in range(3)]
    chunks += [
        chunk_of(4 + n, up_in.at[:, pl.ds(n * part, part)], at_of(wup, n)) for n in range(quarters)
    ]
    last_chunk = len(chunks)
    down = SlabChunk(place, down_in, at_of(wdown), down_send, down_yrecv, down_crecv)
    down_line = Line(last_chunk, place, down_in, at_of(wdown), place.y, sems)
    toward = jnp.where(place.z < line // 2, 1, line - 1)

    def slab_at(order):
        return (place.z + toward * order) % line

    def issue(number):
        chunks[number].issue(over=number >= EARLY)

    def mirror(number):
        if number < last_chunk:
            chunks[number].mirror()
        else:
            down.mirror(slab_at(number - last_chunk))

    def relay(number):
        (*chunks, down_line)[number].relay()

    def forward(number):
        if number < last_chunk:
            chunks[number].forward()
        else:
            slab = slab_at(number - last_chunk)
            down_line.wait_slab(slab)
            down.y_copy(slab, place.y).start()

    def step(number):
        forward(number)
        if number == 1:
            for early in PAIRED:
                chunks[early].y_own().start()
        if number == 4:
            down.y_own().start()
            down.own_copy().start()
        if number + 1 < last_chunk:
            relay(number + 1)
        if number == 5:
            down_line.issue_line(NEAR[::2])
        if number == 6:
            down_line.issue_line(NEAR[1::2])
        for later in ISSUES.get(number, ()):
            issue(later)
        if 1 <= number < 5:
            mirror(number - 1)

    place.greet()
    for number in range(FIRST):
        issue(number)
    for number in range(EARLY):
        chunks[number].y_own().start()
    sent_margin = misc(
        images_in.at[:, pl.ds(images_in.shape[1] - margin_rows, margin_rows)],
        picture.at[:, pl.ds(0, margin_rows)], 0, xpeer,
    )

    @pl.when(side == 0)
    def _():
        sent_margin.start()

    piece = pl.ds(core * half, half)
    other_piece = pl.ds((1 - core) * half, half)
    pos_send = misc(pos_in.at[piece], pos.at[side, piece], 1, xpeer)
    pos_send.start()

    def flat_copy(where, index):
        there = pl.ds(pl.multiple_of(index * flat_rows, flat_rows), flat_rows)
        return misc(flat.at[where, there], flat.at[where, there], 5 + index, xpeer)

    def stem(field, weight_one, first, second, third):
        unroll = largest_divisor(first.shape[0], 16)
        two_columns(kernel_one, weight_one, depth)
        own_picture.wait()
        pick_rows(picture, field, margin_rows, images_in.shape[1], depth)
        relay(0)
        conv_one(field, weight_one, first, 1, first.shape[0] // unroll, unroll, depth, 1)

        @pl.when(side == 0)
        def _():
            picture[:, pl.ds(0, margin_rows)] = jnp.zeros(
                (images_in.shape[0], margin_rows, images_in.shape[2]), picture.dtype
            )

        @pl.when(side == 1)
        def _():
            sent_margin.wait_recv()

        pick_rows(picture, field, 0, margin_rows, depth)
        conv_one(field, weight_one, first, 0, 1, unroll, depth, 1)
        step(0)
        conv_two(first, kernel_two, second, 8)
        fetches[0].wait()
        chunk_three = largest_divisor(third.shape[1], 16)

        def act_three(row):
            made = conv_later(second, kernel_three, chunk_three, row)
            keep(third, row, chunk_three, third.shape[2], made.astype(jnp.float32))

        row_chunks(third.shape[1], chunk_three, act_three)
        fetches[1].wait()
        columns = third.shape[2] // 2

        def act_four(index, carry):
            made = conv_later(third, kernel_four, flat_rows // columns, index * (flat_rows // columns))
            there = pl.ds(pl.multiple_of(index * flat_rows, flat_rows), flat_rows)
            flat[side, there] = made
            flat_copy(side, index).start()
            return carry

        lax.fori_loop(0, flat_parts, act_four, 0)

    out_rows = images_in.shape[1] // 16
    counts = [(((out_rows * 2 + 1) * 2 + 1) * 2 + 1), (out_rows * 2 + 1) * 2 + 1, out_rows * 2 + 1]
    pairs = images_in.shape[2] // 4
    pl.run_scoped(
        stem,
        pltpu.VMEM((picture.shape[1] * depth, pairs), jnp.float32),
        pltpu.VMEM((3 * depth, 2 * kernel_two.shape[2]), jnp.float32),
        pltpu.VMEM((counts[0], pairs, 2 * kernel_two.shape[2]), jnp.bfloat16),
        pltpu.VMEM((kernel_two.shape[3] // LANES, counts[1], pairs, LANES), jnp.float32),
        pltpu.VMEM((kernel_three.shape[3] // LANES, counts[2], pairs // 2, LANES), jnp.float32),
    )
    step(1)
    out_cross = misc(wout.at[:, :, core], wout_other.at[:, :, core], 2, xpeer)
    out_cross.start()

    def embed(where, index):
        own = pl.ds(pl.multiple_of(index * half, half), half)
        chunk = (
            jnp.dot(flat[where, own], proj[...], preferred_element_type=jnp.float32)
            + pos[where, own].astype(jnp.float32)
        ).astype(jnp.bfloat16)
        tokens[where, own] = chunk
        normed[where, own] = norm_rows(chunk, gain_one[...])

    fetches[2].wait()
    fetches[3].wait()
    embed(side, 0)
    embed(side, 1)
    arriving = pos.at[other, piece]
    misc(arriving, arriving, 1, xpeer).wait_recv()
    pos_mirror = misc(arriving, arriving, 3, sibling)
    pos_mirror.start()
    step(2)
    coming = pos.at[other, other_piece]
    misc(coming, coming, 3, sibling).wait_recv()
    for index in range(flat_parts):
        flat_copy(other, index).wait_recv()
    embed(other, 0)
    embed(other, 1)
    step(3)

    cross = wout_other.at[:, :, core]
    out_mirror = misc(cross, cross, 4, sibling)

    def attention(qkv):
        def project(which):
            chunks[1 + which].ready()

            def act(where, carry):
                weight = wqkv[which].reshape(width, heads * head_size)
                made = pair_dot(weight, normed[where], ((0,), (1,)))
                columns = pl.ds(pl.multiple_of(where * rows, rows), rows)
                qkv[which, :, :, columns] = made.astype(jnp.bfloat16).reshape(heads, head_size, rows)
                return carry

            lax.fori_loop(0, 2, act, 0)

        project(0)
        project(1)
        step(4)
        project(2)
        factor = math.log2(math.e) / math.sqrt(head_size)

        def attend_head(index, carry):
            group, head = index // heads, index % heads
            keys, values = qkv[1, head], qkv[2, head]
            for where in range(2):
                columns = pl.ds(pl.multiple_of(where * rows + group * half, half), half)
                query = qkv[0, head, :, columns]
                score = pair_dot(keys, query, ((0,), (0,)))
                top = jnp.max(score, axis=0, keepdims=True)
                weight = jnp.exp2((score - top) * factor)
                below = jnp.sum(weight, axis=0, keepdims=True)
                made = jnp.dot(values, weight.astype(jnp.bfloat16), preferred_element_type=jnp.float32)
                made = (made / below).astype(jnp.bfloat16)
                mixed[side, group, head, :, where * half : (where + 1) * half] = made
            mix_copy(side, index).start()

            @pl.when(index == heads // 2 - 1)
            def _():
                misc(cross, cross, 2, xpeer).wait_recv()
                out_mirror.start()

            for number, when in PLACED:
                @pl.when(index == heads * when // 8)
                def _():
                    step(number)

            return carry

        lax.fori_loop(0, 2 * heads, attend_head, 0)

    def mix_copy(share_of, index):
        there = mixed.at[share_of, index // heads, index % heads]
        return remote(there, there, mix_send.at[index], mix_recv.at[index], xpeer)

    pl.run_scoped(attention, pltpu.VMEM((3, heads, head_size, count), jnp.bfloat16))
    mirror(4)
    mirror(5)
    forward(last_chunk + 1)
    mirror(last_chunk)
    chunks[0].ready()
    cross_other = wout_other.at[:, :, 1 - core]
    misc(cross_other, cross_other, 4, sibling).wait_recv()

    def settle(index, carry):
        group, where = index // 2, index % 2
        own = pl.ds(pl.multiple_of(group * half, half), half)
        columns = pl.ds(pl.multiple_of(where * half, half), half)
        attn = tokens[where, own].astype(jnp.float32)
        for share_of, weight in ((side, wout), (other, wout_other)):
            left = mixed[share_of, group, :, :, columns].reshape(heads * head_size, half)
            share = pair_dot(left, weight[...].reshape(width, heads * head_size), ((0,), (1,)))
            attn = attn + share.astype(jnp.bfloat16).astype(jnp.float32)
        chunk = attn.astype(jnp.bfloat16)
        tokens[where, own] = chunk
        normed[where, own] = norm_rows(chunk, gain_two[...])
        return carry

    slab_rows = width // line

    def back_copy(slab, group):
        there = pl.ds(pl.multiple_of(slab * slab_rows, slab_rows), slab_rows)
        lanes = pl.ds(group * half, half)
        return remote(
            back.at[there, lanes], arrived.at[there, lanes],
            back_send.at[slab, group], back_recv.at[slab, group], xpeer,
        )

    def feed(hidden, total):
        def rise(group):
            own = pl.ds(group * half, half)

            def act(quarter, carry):
                weight = wup[quarter].reshape(width, part)
                before = jnp.dot(
                    normed[:, own].reshape(2 * half, width), weight, preferred_element_type=jnp.float32
                )
                made = 0.5 * before * (1.0 + lax.erf(before * math.sqrt(0.5)))
                there = pl.ds(pl.multiple_of(quarter * part, part), part)
                hidden[:, own, there] = made.astype(jnp.bfloat16).reshape(2, half, part)
                return carry

            lax.fori_loop(0, quarters, act, 0)

        def weight_of(order):
            slab = slab_at(order)
            there = pl.ds(pl.multiple_of(slab * slab_rows, slab_rows), slab_rows)
            return slab, there, wdown[slab].reshape(slab_rows, units)

        def give(order, group):
            slab, there, weight = weight_of(order)
            own = pl.ds(group * half, half)
            back[there, own] = pair_dot(weight, hidden[other, own], ((1,), (1,))).astype(jnp.bfloat16)
            back_copy(slab, group).start()

        def fall(order):
            slab, there, weight = weight_of(order)
            total[there] = pair_dot(weight, hidden[side], ((1,), (1,))).astype(jnp.bfloat16)

        def meet(group):
            for head in range(heads):
                mix_copy(other, group * heads + head).wait_recv()
            lax.fori_loop(2 * group, 2 * group + 2, settle, 0)

        mirror(6)
        mirror(7)
        meet(0)
        relay(last_chunk)
        forward(last_chunk + 2)
        for quarter in range(quarters):
            chunks[4 + quarter].ready()
        rise(0)
        down.ready(slab_at(0))
        give(0, 0)
        mirror(last_chunk + 1)
        down.ready(slab_at(1))
        give(1, 0)
        forward(last_chunk + 3)
        meet(1)
        rise(1)
        mirror(last_chunk + 2)
        give(0, 1)
        give(1, 1)
        fall(0)
        down.ready(slab_at(2))
        give(2, 0)
        give(2, 1)
        for order in range(4, line):
            forward(last_chunk + order)
        fall(1)
        for order in range(3, line):
            mirror(last_chunk + order)
        for order in range(3, line):
            down.ready(slab_at(order))
            give(order, 0)
            give(order, 1)
        for order in range(2, line):
            fall(order)
        for slab in range(line):
            for group in range(2):
                back_copy(slab, group).wait_recv()
        summed = total[...].astype(jnp.float32) + arrived[...].astype(jnp.float32)
        encoded[...] = (tokens[side].astype(jnp.float32) + summed.T).astype(jnp.bfloat16)

    pl.run_scoped(
        feed, pltpu.VMEM((2, rows, units), jnp.bfloat16), pltpu.VMEM((width, rows), jnp.bfloat16)
    )

    @pl.when(side == 0)
    def _():
        sent_margin.wait_send()

    for copy in (pos_send, out_cross, pos_mirror, out_mirror):
        copy.wait_send()
    for index in range(flat_parts):
        flat_copy(side, index).wait_send()
    for index in range(2 * heads):
        mix_copy(side, index).wait_send()
    for slab in range(line):
        for group in range(2):
            back_copy(slab, group).wait_send()
    for chunk in chunks:
        chunk.drain()
    down_line.drain_line()
    down.drain()


def whole_block(
    images, pos, kernel_one, kernel_two, kernel_three, kernel_four, proj, gain_one, gain_two,
    qkv_shard, out_shard, up_shard, down_shard,
):
    line = lax.axis_size("dp") // 4
    depth, local, units = qkv_shard.shape[1], qkv_shard.shape[2], up_shard.shape[1]
    rows, width = pos.shape
    head_size = width // HEADS
    heads = local // head_size
    quarters = 4
    numbers = 5 + quarters + len(PAIRED)
    whole = 4 + quarters
    here = (line, 2, 2, depth)
    bf16 = jnp.bfloat16
    vmem = pl.BlockSpec(memory_space=pltpu.VMEM)
    hbm = pl.BlockSpec(memory_space=pl.ANY)
    dma = pltpu.SemaphoreType.DMA
    return pl.pallas_call(
        functools.partial(block_body, line, head_size),
        out_shape=jax.ShapeDtypeStruct((rows, width), bf16),
        in_specs=[hbm, vmem, vmem, hbm, hbm, hbm, hbm, vmem, vmem, hbm, hbm, hbm, hbm],
        out_specs=vmem,
        scratch_shapes=[
            pltpu.VMEM((images.shape[1], images.shape[2] + 16, images.shape[3]), bf16),
            pltpu.VMEM(kernel_three.shape, bf16),
            pltpu.VMEM(kernel_four.shape, bf16),
            pltpu.VMEM(proj.shape, bf16),
            pltpu.VMEM((2, rows, proj.shape[0]), bf16),
            pltpu.VMEM((2, rows, width), bf16),
            pltpu.VMEM((2, rows, width), bf16),
            pltpu.VMEM((2, rows, width), bf16),
            pltpu.VMEM((3, *here, local), bf16),
            pltpu.VMEM((*here, local), bf16),
            pltpu.VMEM((*here, local), bf16),
            pltpu.VMEM((quarters, *here, units // quarters), bf16),
            pltpu.VMEM((*here, units), bf16),
            pltpu.VMEM((2, 2, heads, head_size, rows), bf16),
            pltpu.VMEM((width, rows), bf16),
            pltpu.VMEM((width, rows), bf16),
            dma((numbers, 4 + 2 * (line - 3))),
            dma((numbers, line)),
            dma((whole,)),
            dma((whole,)),
            dma((whole,)),
            dma((whole,)),
            dma((whole,)),
            dma((3,)),
            dma((line,)),
            dma((line,)),
            dma((7,)),
            dma((7,)),
            dma((5,)),
            dma((2 * heads,)),
            dma((2 * heads,)),
            dma((line, 2)),
            dma((line, 2)),
        ],
        compiler_params=pltpu.CompilerParams(
            collective_id=0, has_side_effects=True, vmem_limit_bytes=VMEM_LIMIT
        ),
    )(
        images[0], kernel_one, kernel_two, kernel_three, kernel_four, pos, proj, gain_one, gain_two,
        qkv_shard, out_shard, up_shard, down_shard,
    )


def on_ring(
    images,
    pos_embed,
    conv_first,
    conv_second,
    conv_third,
    conv_fourth,
    proj_weight,
    ln_first,
    qkv_weight,
    out_weight,
    ln_second,
    up_weight,
    down_weight,
):
    count = lax.axis_size("space")
    attention_part = gathered(
        jnp.concatenate([jnp.moveaxis(qkv_weight, 1, 0), out_weight.T[None]], axis=0), 1
    )
    feed_part = gathered(jnp.stack([up_weight, down_weight.T]), 1)
    out_part = attention_part[3]
    up_part, down_part = feed_part[0], feed_part[1]
    margin = passed_along(images[:, :, -15:, :], "space", 1)
    positions = [pos_embed] + [shifted(pos_embed, "space", k) for k in range(1, count)]

    stem_out = second_conv(first_conv(images, margin, conv_first), conv_second)
    for kernel in (conv_third, conv_fourth):
        stem_out = later_conv(stem_out, kernel)
    flat = stem_out.reshape(-1, stem_out.shape[3])
    flats = [flat] + [shifted(flat, "space", k) for k in range(1, count)]
    width = proj_weight.shape[1]
    local = attention_part.shape[2]
    head_size = width // HEADS

    tokens = None
    projected = []
    for rows, position in zip(flats, positions):
        chunk = (
            jnp.dot(rows, proj_weight, preferred_element_type=jnp.float32)
            + position.astype(jnp.float32)
        ).astype(jnp.bfloat16)
        tokens = chunk if tokens is None else tokens
        normed = layer_norm(chunk, ln_first)
        projected.append(
            [
                lax.dot_general(
                    attention_part[which],
                    normed,
                    (((0,), (1,)), ((), ())),
                    preferred_element_type=jnp.float32,
                ).astype(jnp.bfloat16)
                for which in range(3)
            ]
        )
    keys = [part[1] for part in projected]
    values = [part[2] for part in projected]

    def attention_share(query):
        mixed = attend(query, keys, values, head_size)
        share = lax.dot_general(
            mixed, out_part, (((0,), (1,)), ((), ())), preferred_element_type=jnp.float32
        ).astype(jnp.bfloat16)
        return mixed, share

    returned = []
    last = None
    for k in list(range(1, count)) + [0]:
        query = projected[k][0]
        if last is not None:
            query, _ = lax.optimization_barrier((query, last))
        last, share = attention_share(query)
        returned.append(shifted(share, "space", -k) if k else share)
    attn_sum = sum(part.astype(jnp.float32) for part in returned)
    after_attn = (tokens.astype(jnp.float32) + attn_sum).astype(jnp.bfloat16)
    normed_two = layer_norm(after_attn, ln_second)

    def feed_forward(rows):
        before = jnp.dot(rows, up_part, preferred_element_type=jnp.float32)
        hidden = (0.5 * before * (1.0 + lax.erf(before * math.sqrt(0.5)))).astype(jnp.bfloat16)
        hidden = lax.optimization_barrier(hidden)
        return lax.dot_general(
            hidden, down_part, (((1,), (1,)), ((), ())), preferred_element_type=jnp.float32
        ).astype(jnp.bfloat16)

    rows = normed_two.shape[0]
    half = rows // 2
    pieces = [normed_two[:half], normed_two[half:]]
    moved = [[shifted(piece, "space", k) for piece in pieces] for k in range(1, count)]
    totals = feed_forward(normed_two).astype(jnp.float32)
    back = [
        jnp.concatenate([shifted(feed_forward(piece), "space", -k) for piece in there], axis=0)
        for k, there in zip(range(1, count), moved)
    ]
    for part in back:
        totals = totals + part.astype(jnp.float32)
    return (after_attn.astype(jnp.float32) + totals).astype(jnp.bfloat16)[None]


def on_device(
    images,
    pos_embed,
    conv_first,
    conv_second,
    conv_third,
    conv_fourth,
    proj_weight,
    ln_first,
    qkv_weight,
    out_weight,
    ln_second,
    up_weight,
    down_weight,
):
    shards = lax.axis_size("dp")
    fits = lax.axis_size("space") == 2 and shards % 16 == 0 and images.shape[0] == 1
    fits = fits and qkv_weight.shape[0] % 16 == 0 and qkv_weight.shape[2] % 128 == 0
    if not fits:
        return on_ring(
            images, pos_embed, conv_first, conv_second, conv_third, conv_fourth, proj_weight,
            ln_first, qkv_weight, out_weight, ln_second, up_weight, down_weight,
        )
    out = whole_block(
        images, pos_embed, conv_first, conv_second, conv_third, conv_fourth, proj_weight,
        ln_first, ln_second,
        jnp.moveaxis(qkv_weight, 1, 0), out_weight.T, up_weight, down_weight.T,
    )
    return out[None]


def solution(mesh):
    placed = (
        P("dp", None, "space", None),
        P("space", None),
        P(),
        P(),
        P(),
        P(),
        P(),
        P(),
        P("dp", None, "space"),
        P("space", "dp"),
        P(),
        P("dp", "space"),
        P("space", "dp"),
    )
    return jax.shard_map(
        on_device, mesh=mesh, in_specs=placed, out_specs=P("dp", "space", None), check_vma=False
    )
```

```python
import functools
import math

import jax
import jax.numpy as jnp
from jax import lax
from jax.experimental import pallas as pl
from jax.experimental.pallas import tpu as pltpu
from jax.sharding import PartitionSpec as P

HEADS = 16
PHASES = 5


def passed_along(value, axis, steps):
    count = lax.axis_size(axis)
    leading, last = (max(0, -steps), min(count, count - steps))
    return lax.ppermute(value, axis, [(source, source + steps) for source in range(leading, last)])


def shifted(value, axis, steps):
    count = lax.axis_size(axis)
    return lax.ppermute(value, axis, [(source, (source + steps) % count) for source in range(count)])


def largest_divisor(number, limit):
    return max(d for d in range(1, limit + 1) if number % d == 0)


def first_conv_body(unroll, field_ref, kernel_ref, out_ref):
    depth = field_ref.shape[1]
    lanes = field_ref.shape[2]

    def step(index, carry):
        for part in range(unroll):
            row = index * unroll + part
            patch = field_ref[pl.ds(2 * row, 3)].reshape(3 * depth, lanes)
            out = lax.dot_general(
                patch, kernel_ref[...], (((0,), (0,)), ((), ())), preferred_element_type=jnp.float32
            )
            out_ref[row] = jnp.maximum(out, 0.0).astype(out_ref.dtype)
        return carry

    lax.fori_loop(0, out_ref.shape[0] // unroll, step, 0)


def first_conv(images, margin, kernel):
    wide = images.shape[3]
    pairs = wide // 4
    channels = images.shape[1]
    out_channels = kernel.shape[3]
    source = lax.broadcasted_iota(jnp.int32, (wide, PHASES, pairs), 0)
    phase = lax.broadcasted_iota(jnp.int32, (wide, PHASES, pairs), 1)
    pair = lax.broadcasted_iota(jnp.int32, (wide, PHASES, pairs), 2)
    pick = (source == 4 * pair + phase - 1).astype(jnp.bfloat16)
    field = jnp.concatenate([margin, images], axis=2)[0]
    rows = field.shape[1]
    picked = jnp.einsum("chw,wqp->hcqp", field, pick, preferred_element_type=jnp.float32)
    picked = picked.astype(jnp.bfloat16).reshape(rows, channels * PHASES, pairs)
    depth = -(-channels * PHASES // 16) * 16
    picked = jnp.pad(picked, ((0, 0), (0, depth - channels * PHASES), (0, 0)))
    taps = jnp.transpose(kernel, (0, 2, 1, 3))
    left = jnp.pad(taps, ((0, 0), (0, 0), (0, 2), (0, 0)))
    right = jnp.pad(taps, ((0, 0), (0, 0), (2, 0), (0, 0)))
    both = jnp.concatenate([left, right], axis=3).reshape(3, channels * PHASES, 2 * out_channels)
    both = jnp.pad(both, ((0, 0), (0, depth - channels * PHASES), (0, 0)))
    both = both.reshape(3 * depth, 2 * out_channels)
    count = (rows - 3) // 2 + 1
    out = pl.pallas_call(
        functools.partial(first_conv_body, largest_divisor(count, 16)),
        out_shape=jax.ShapeDtypeStruct((count, pairs, 2 * out_channels), jnp.bfloat16),
        in_specs=[pl.BlockSpec(memory_space=pltpu.VMEM)] * 2,
        out_specs=pl.BlockSpec(memory_space=pltpu.VMEM),
        compiler_params=pltpu.CompilerParams(vmem_limit_bytes=40 * 1024 * 1024),
        cost_estimate=pl.CostEstimate(
            flops=count * pairs * depth * 3 * 4 * out_channels * 4,
            bytes_accessed=count * pairs * out_channels * 4,
            transcendentals=0,
        ),
    )(picked, both)
    return out[None]


def second_conv(field, kernel):
    height, _, inner, outer = kernel.shape
    before = jnp.concatenate([jnp.zeros_like(kernel[:, 0]), kernel[:, 0]], axis=1)
    here = jnp.concatenate([kernel[:, 1], kernel[:, 2]], axis=1)
    paired = jnp.stack([before, here], axis=1)
    out = lax.conv_general_dilated(
        field,
        paired,
        (2, 1),
        ((0, 0), (1, 0)),
        dimension_numbers=("NHWC", "HWIO", "NHWC"),
        preferred_element_type=jnp.float32,
    )
    return jax.nn.relu(out).astype(jnp.bfloat16)


def later_conv(field, kernel):
    out = lax.conv_general_dilated(
        field,
        kernel,
        (2, 2),
        ((0, 0), (1, 1)),
        dimension_numbers=("NHWC", "HWIO", "NHWC"),
        preferred_element_type=jnp.float32,
    )
    return jax.nn.relu(out).astype(jnp.bfloat16)


def layer_norm(values, gain):
    wide = values.astype(jnp.float32)
    center = wide - jnp.mean(wide, axis=-1, keepdims=True)
    spread = jnp.mean(center * center, axis=-1, keepdims=True)
    return (center * lax.rsqrt(spread + 1e-06) * gain).astype(jnp.bfloat16)


def attend_body(chunks, factor, *refs):
    query_ref, out_ref = refs[0], refs[-1]
    keys, values = refs[1 : 1 + chunks], refs[1 + chunks : 1 + 2 * chunks]
    total = query_ref.shape[1]
    block = largest_divisor(total // 128, 2) * 128
    for start in range(0, total, block):
        query = query_ref[:, start : start + block]
        scores = [
            lax.dot_general(
                key[...], query, (((0,), (0,)), ((), ())), preferred_element_type=jnp.float32
            )
            for key in keys
        ]
        top = functools.reduce(
            jnp.maximum, [jnp.max(score, axis=0, keepdims=True) for score in scores]
        )
        weights = [jnp.exp2((score - top) * factor) for score in scores]
        below = sum(jnp.sum(weight, axis=0, keepdims=True) for weight in weights)
        mixed = sum(
            jnp.dot(value[...], weight.astype(jnp.bfloat16), preferred_element_type=jnp.float32)
            for value, weight in zip(values, weights)
        )
        out_ref[:, start : start + block] = (mixed / below).astype(out_ref.dtype)


def attend(query, keys, values, head_size):
    local, total = query.shape
    chunks = len(keys)
    seen = sum(key.shape[1] for key in keys)
    spec = lambda array: pl.BlockSpec((head_size, array.shape[1]), lambda head: (head, 0))
    factor = math.log2(math.e) / math.sqrt(head_size)
    return pl.pallas_call(
        functools.partial(attend_body, chunks, factor),
        grid=(local // head_size,),
        out_shape=jax.ShapeDtypeStruct((local, total), jnp.bfloat16),
        in_specs=[spec(array) for array in (query, *keys, *values)],
        out_specs=spec(query),
        compiler_params=pltpu.CompilerParams(vmem_limit_bytes=40 * 1024 * 1024),
        cost_estimate=pl.CostEstimate(
            flops=local * total * seen * 16,
            bytes_accessed=local * (2 * total + 2 * seen) * 2,
            transcendentals=(local // head_size) * total * seen,
        ),
    )(query, *keys, *values)


def gathered(weight, axis):
    return lax.all_gather(weight, "dp", axis=axis, tiled=True)


MESH = pl.DeviceIdType.MESH
VMEM_LIMIT = 63 * 1024 * 1024
FIRST = 2
ISSUES = {0: (2,), 1: (3, 4), 2: (5,), 3: (6,), 4: (7,)}
EARLY = 7
PLACED = ((5, 2), (6, 8), (7, 14))
PAIRED = ()
LANES = 128
NEAR = (1, 2, -1, -2)


def norm_rows(values, gain):
    wide = values.astype(jnp.float32)
    center = wide - jnp.mean(wide, axis=-1, keepdims=True)
    spread = jnp.mean(center * center, axis=-1, keepdims=True)
    return (center * lax.rsqrt(spread + 1e-06) * gain).astype(jnp.bfloat16)


def pair_dot(left, right, dims):
    return lax.dot_general(left, right, (dims, ((), ())), preferred_element_type=jnp.float32)


def remote(source, target, send, recv, device):
    return pltpu.make_async_remote_copy(
        src_ref=source, dst_ref=target, send_sem=send, recv_sem=recv,
        device_id=device, device_id_type=MESH,
    )


class Place:
    def __init__(self, line):
        self.line = line
        me, self.side = lax.axis_index("dp"), lax.axis_index("space")
        self.core, self.y, self.z = me % 2, (me // 2) % 2, me // 4
        self.sibling = {"dp": me + 1 - 2 * self.core, "space": self.side}
        self.ypeer = {"dp": me + 2 - 4 * self.y, "space": self.side}
        self.xpeer = {"dp": me, "space": 1 - self.side}

    def on_line(self, step):
        return {"dp": (self.z + step) * 4 + self.y * 2 + self.core, "space": self.side}

    def each_near(self, act, steps=NEAR):
        for step in steps:
            @pl.when((self.z + step >= 0) & (self.z + step < self.line))
            def _():
                act(step)

    def greet(self):
        barrier = pltpu.get_barrier_semaphore()

        def signal(device):
            pl.semaphore_signal(barrier, inc=1, device_id=device, device_id_type=MESH)

        for device in (self.sibling, self.ypeer, self.xpeer):
            signal(device)
        self.each_near(lambda step: signal(self.on_line(step)))
        before = jnp.minimum(self.z, 2)
        behind = jnp.minimum(self.line - 1 - self.z, 2)
        pl.semaphore_wait(barrier, 3 + before + behind)


class Line:
    def __init__(self, number, place, source, at, row, sems):
        self.number, self.place, self.at, self.row = number, place, at, row
        self.zsend, self.zrecv = sems[:2]
        self.mine = at(place.z, row, place.core)
        self.source = self.mine if source is None else source

    def z_copy(self, step):
        n, p = self.number, self.place
        return remote(
            self.source, self.mine, self.zsend.at[n, NEAR.index(step)], self.zrecv.at[n, p.z],
            p.on_line(step),
        )

    def z_further(self, slab, step):
        n, p = self.number, self.place
        here = self.at(slab, self.row, p.core)
        slot = 4 + slab if step > 0 else p.line + p.line - slab
        return remote(here, here, self.zsend.at[n, slot], self.zrecv.at[n, slab], p.on_line(step))

    def each_further(self, act):
        p = self.place
        for slab in range(p.line - 3):
            @pl.when((p.z - slab >= 2) & (p.z + 1 < p.line))
            def _():
                act(slab, self.z_further(slab, 1))

        for slab in range(3, p.line):
            @pl.when((slab - p.z >= 2) & (p.z >= 1))
            def _():
                act(slab, self.z_further(slab, -1))

    def passes_on(self, slab):
        p = self.place
        return ((p.z - slab >= 2) & (p.z + 1 < p.line)) | ((slab - p.z >= 2) & (p.z >= 1))

    def arrived(self, slab):
        p = self.place
        here = self.at(slab, self.row, p.core)
        remote(
            here, here, self.zsend.at[self.number, 0], self.zrecv.at[self.number, slab], p.ypeer
        ).wait_recv()

    def issue_line(self, steps=NEAR):
        self.place.each_near(lambda step: self.z_copy(step).start(), steps)

    def relay(self):
        def act(slab, copy):
            self.arrived(slab)
            copy.start()

        self.each_further(act)

    def wait_slab(self, slab):
        @pl.when((slab != self.place.z) & jnp.logical_not(self.passes_on(slab)))
        def _():
            self.arrived(slab)

    def wait_line(self):
        for slab in range(self.place.line):
            self.wait_slab(slab)

    def drain_line(self):
        self.place.each_near(lambda step: self.z_copy(step).wait_send())
        self.each_further(lambda slab, copy: copy.wait_send())


class Chunk(Line):
    def __init__(self, number, place, source, at, sems):
        super().__init__(number, place, source, at, place.y, sems)
        self.ysend, self.yrecv, self.csend, self.crecv, self.local = [
            ref.at[number] for ref in sems[2:]
        ]

    def own_copy(self):
        return pltpu.make_async_copy(self.source, self.mine, self.local)

    def y_own(self):
        return remote(self.source, self.mine, self.ysend, self.yrecv, self.place.ypeer)

    def y_part(self, slab, row):
        here = self.at(slab, row, self.place.core)
        return remote(here, here, self.ysend, self.yrecv, self.place.ypeer)

    def core_part(self, core):
        here = self.at(slice(None), slice(None), core)
        return remote(here, here, self.csend, self.crecv, self.place.sibling)

    def issue(self, over):
        self.own_copy().start()
        self.issue_line()
        if over:
            self.y_own().start()

    def forward(self):
        for slab in range(self.place.line):
            self.wait_slab(slab)

            @pl.when(slab != self.place.z)
            def _():
                self.y_part(slab, self.place.y).start()

    def mirror(self):
        self.own_copy().wait()
        self.y_part(slice(None), 1 - self.place.y).wait_recv()
        self.core_part(self.place.core).start()

    def ready(self):
        self.core_part(1 - self.place.core).wait_recv()

    def drain(self):
        self.drain_line()
        self.y_part(slice(None), self.place.y).wait_send()
        self.core_part(self.place.core).wait_send()


class PairChunk(Chunk):
    def __init__(self, number, second, place, source, at, sems):
        super().__init__(number, place, source, at, sems)
        self.second = Line(second, place, None, at, 1 - place.y, sems)

    def issue(self, over):
        self.own_copy().start()
        self.issue_line()
        self.y_part(self.place.z, 1 - self.place.y).wait_recv()
        self.second.issue_line()

    def relay(self):
        super().relay()
        self.second.relay()

    def forward(self):
        self.wait_line()
        self.second.wait_line()

    def mirror(self):
        self.own_copy().wait()
        self.core_part(self.place.core).start()

    def drain(self):
        self.drain_line()
        self.second.drain_line()
        self.y_own().wait_send()
        self.core_part(self.place.core).wait_send()


class SlabChunk:
    def __init__(self, place, source, at, send, yrecv, crecv):
        self.place, self.source, self.at = place, source, at
        self.send, self.yrecv, self.crecv = send, yrecv, crecv
        self.mine = at(place.z, place.y, place.core)

    def own_copy(self):
        return pltpu.make_async_copy(self.source, self.mine, self.send.at[2])

    def y_own(self):
        z = self.place.z
        return remote(self.source, self.mine, self.send.at[0], self.yrecv.at[z], self.place.ypeer)

    def y_copy(self, slab, row):
        here = self.at(slab, row, self.place.core)
        return remote(here, here, self.send.at[0], self.yrecv.at[slab], self.place.ypeer)

    def core_copy(self, slab, core):
        here = self.at(slab, slice(None), core)
        return remote(here, here, self.send.at[1], self.crecv.at[slab], self.place.sibling)

    def mirror(self, slab):
        @pl.when(slab == self.place.z)
        def _():
            self.own_copy().wait()

        self.y_copy(slab, 1 - self.place.y).wait_recv()
        self.core_copy(slab, self.place.core).start()

    def ready(self, slab):
        self.core_copy(slab, 1 - self.place.core).wait_recv()

    def drain(self):
        p = self.place
        whole = self.at(slice(None), p.y, p.core)
        remote(whole, whole, self.send.at[0], self.yrecv.at[0], p.ypeer).wait_send()
        whole = self.at(slice(None), slice(None), p.core)
        remote(whole, whole, self.send.at[1], self.crecv.at[0], p.sibling).wait_send()


def after_shift(values, period):
    row = lax.broadcasted_iota(jnp.int32, values.shape, 0)
    return jnp.where(row % period == 0, 0.0, pltpu.roll(values, 1, 0))


def row_chunks(total, chunk, act):
    def step(index, carry):
        act(jnp.minimum(index * chunk, total - chunk))
        return carry

    lax.fori_loop(0, -(-total // chunk), step, 0)


def keep(target, row, chunk, columns, made):
    for group in range(target.shape[0]):
        lanes = made[:, group * LANES : (group + 1) * LANES]
        target[group, pl.ds(row, chunk)] = lanes.reshape(chunk, columns, LANES)


def pick_rows(picture, field, start, count, depth):
    channels, wide = picture.shape[0], picture.shape[2]
    pairs = wide // 4
    source = lax.broadcasted_iota(jnp.int32, (wide, pairs), 0)
    pair = lax.broadcasted_iota(jnp.int32, (wide, pairs), 1)
    picks = [
        jnp.where(source == 4 * pair + phase - 1, 1.0, 0.0).astype(jnp.bfloat16)
        for phase in range(PHASES)
    ]
    pick = jnp.concatenate(picks, axis=1)
    for channel in range(channels):
        made = jnp.dot(
            picture[channel, start : start + count], pick, preferred_element_type=jnp.float32
        )
        for phase in range(PHASES):
            rows = pl.ds(start * depth + channel * PHASES + phase, count, stride=depth)
            field[rows, :] = made[:, phase * pairs : (phase + 1) * pairs]
    for spare in range(channels * PHASES, depth):
        rows = pl.ds(start * depth + spare, count, stride=depth)
        field[rows, :] = jnp.zeros((count, pairs), jnp.float32)


def two_columns(kernel, target, depth):
    taps, channels, wide = kernel.shape[0], kernel.shape[2], kernel.shape[3]
    nothing = jnp.zeros((1, wide), jnp.float32)
    target[...] = jnp.zeros_like(target)
    for tap in range(taps):
        columns = [kernel[tap, column].astype(jnp.float32) for column in range(kernel.shape[1])]
        for channel in range(channels):
            pieces = [column[channel : channel + 1] for column in columns]
            for phase in range(PHASES):
                left = pieces[phase] if phase < 3 else nothing
                right = pieces[phase - 2] if phase >= 2 else nothing
                row = tap * depth + channel * PHASES + phase
                target[row : row + 1] = jnp.concatenate([left, right], axis=1)


def conv_one(field, kernel, first, start, stop, unroll, depth, skipped):
    def step(index, carry):
        weight = kernel[...].astype(jnp.bfloat16)
        for part in range(unroll):
            row = index * unroll + part
            begin = pl.multiple_of((2 * row + skipped) * depth, depth)
            patch = field[pl.ds(begin, 3 * depth)].astype(jnp.bfloat16)
            out = pair_dot(patch, weight, ((0,), (0,)))
            first[row] = jnp.maximum(out, 0.0).astype(first.dtype)
        return carry

    lax.fori_loop(start, stop, step, 0)


def conv_two(first, kernel, second, chunk):
    total, columns = second.shape[1], first.shape[1]
    deep, wide = kernel.shape[2], kernel.shape[3]

    def act(row):
        parts, weights = [], []
        for tap in range(3):
            parts.append(jnp.concatenate([first[2 * (row + n) + tap] for n in range(chunk)], axis=0))
            before = jnp.concatenate([jnp.zeros((deep, wide), jnp.bfloat16), kernel[tap, 0]], axis=0)
            here = jnp.concatenate([kernel[tap, 1], kernel[tap, 2]], axis=0)
            weights.append(jnp.concatenate([before, here], axis=1))
        made = jnp.dot(
            jnp.concatenate(parts, axis=1), jnp.concatenate(weights, axis=0),
            preferred_element_type=jnp.float32,
        )
        out = made[:, wide:] + after_shift(made[:, :wide], columns)
        out = jnp.maximum(out, 0.0).astype(jnp.bfloat16).astype(jnp.float32)
        keep(second, row, chunk, columns, out)

    row_chunks(total, chunk, act)


def conv_later(source, kernel, chunk, row):
    columns = source.shape[2] // 2
    deep, wide = kernel.shape[2], kernel.shape[3]
    out, moved = None, None
    for tap in range(3):
        even, odd = [
            jnp.concatenate(
                [
                    jnp.concatenate(
                        [
                            source[group, 2 * (row + n) + tap, pl.ds(phase, columns, stride=2), :]
                            for n in range(chunk)
                        ],
                        axis=0,
                    )
                    for group in range(source.shape[0])
                ],
                axis=1,
            ).astype(jnp.bfloat16)
            for phase in range(2)
        ]
        here = jnp.concatenate([kernel[tap, 1], kernel[tap, 2]], axis=0)
        both = jnp.concatenate([even, odd], axis=1)
        made = jnp.dot(both, here, preferred_element_type=jnp.float32)
        late = jnp.dot(odd, kernel[tap, 0], preferred_element_type=jnp.float32)
        out = made if out is None else out + made
        moved = late if moved is None else moved + late
    return jnp.maximum(out + after_shift(moved, columns), 0.0).astype(jnp.bfloat16)


def block_body(
    line, head_size,
    images_in, kernel_one, kernel_two, kernel_three_in, kernel_four_in,
    pos_in, proj_in, gain_one, gain_two, qkv_in, out_in, up_in, down_in,
    encoded,
    picture, kernel_three, kernel_four, proj, flat, pos, tokens, normed,
    wqkv, wout, wout_other, wup, wdown, mixed, back, arrived,
    zsend, zrecv, ysend, yrecv, csend, crecv, local, down_send, down_yrecv, down_crecv, misc_send, misc_recv, misc_local,
    mix_send, mix_recv, back_send, back_recv,
):
    place = Place(line)
    side, core = place.side, place.core
    other = 1 - side
    xpeer, sibling = place.xpeer, place.sibling
    sems = (zsend, zrecv, ysend, yrecv, csend, crecv, local)
    rows, width = tokens.shape[1], tokens.shape[2]
    half = rows // 2
    count = 2 * rows
    units = up_in.shape[1]
    quarters = wup.shape[0]
    part = units // quarters
    heads = mixed.shape[2]
    margin_rows = picture.shape[1] - images_in.shape[1]
    depth = -(-images_in.shape[0] * PHASES // 16) * 16
    flat_parts = 2
    flat_rows = rows // flat_parts

    def misc(source, target, slot, device):
        return remote(source, target, misc_send.at[slot], misc_recv.at[slot], device)

    def fetch(source, target, slot):
        return pltpu.make_async_copy(source, target, misc_local.at[slot])

    own_rows = pl.ds(margin_rows, images_in.shape[1])
    own_picture = fetch(images_in, picture.at[:, own_rows], 0)
    own_picture.start()
    fetches = [
        fetch(kernel_three_in, kernel_three, 1),
        fetch(kernel_four_in, kernel_four, 2),
        fetch(proj_in, proj, 3),
        fetch(pos_in, pos.at[side], 4),
    ]
    for copy in fetches:
        copy.start()

    def at_of(ref, *lead):
        return lambda a, b, c: ref.at[(*lead, a, b, c)]

    def chunk_of(number, source, at):
        if number in PAIRED:
            second = 5 + quarters + PAIRED.index(number)
            return PairChunk(number, second, place, source, at, sems)
        return Chunk(number, place, source, at, sems)

    chunks = [chunk_of(0, out_in, at_of(wout))]
    chunks += [chunk_of(1 + n, qkv_in.at[n], at_of(wqkv, n)) for n in range(3)]
    chunks += [
        chunk_of(4 + n, up_in.at[:, pl.ds(n * part, part)], at_of(wup, n)) for n in range(quarters)
    ]
    last_chunk = len(chunks)
    down = SlabChunk(place, down_in, at_of(wdown), down_send, down_yrecv, down_crecv)
    down_line = Line(last_chunk, place, down_in, at_of(wdown), place.y, sems)
    toward = jnp.where(place.z < line // 2, 1, line - 1)

    def slab_at(order):
        return (place.z + toward * order) % line

    def issue(number):
        chunks[number].issue(over=number >= EARLY)

    def mirror(number):
        if number < last_chunk:
            chunks[number].mirror()
        else:
            down.mirror(slab_at(number - last_chunk))

    def relay(number):
        (*chunks, down_line)[number].relay()

    def forward(number):
        if number < last_chunk:
            chunks[number].forward()
        else:
            slab = slab_at(number - last_chunk)
            down_line.wait_slab(slab)
            down.y_copy(slab, place.y).start()

    def step(number):
        forward(number)
        if number == 1:
            for early in PAIRED:
                chunks[early].y_own().start()
        if number == 4:
            down.y_own().start()
            down.own_copy().start()
        if number + 1 < last_chunk:
            relay(number + 1)
        if number == 5:
            down_line.issue_line(NEAR[::2])
        if number == 6:
            down_line.issue_line(NEAR[1::2])
        for later in ISSUES.get(number, ()):
            issue(later)
        if 1 <= number < 5:
            mirror(number - 1)

    place.greet()
    for number in range(FIRST):
        issue(number)
    for number in range(EARLY):
        chunks[number].y_own().start()
    sent_margin = misc(
        images_in.at[:, pl.ds(images_in.shape[1] - margin_rows, margin_rows)],
        picture.at[:, pl.ds(0, margin_rows)], 0, xpeer,
    )

    @pl.when(side == 0)
    def _():
        sent_margin.start()

    piece = pl.ds(core * half, half)
    other_piece = pl.ds((1 - core) * half, half)
    pos_send = misc(pos_in.at[piece], pos.at[side, piece], 1, xpeer)
    pos_send.start()

    def flat_copy(where, index):
        there = pl.ds(pl.multiple_of(index * flat_rows, flat_rows), flat_rows)
        return misc(flat.at[where, there], flat.at[where, there], 5 + index, xpeer)

    def stem(field, weight_one, first, second, third):
        unroll = largest_divisor(first.shape[0], 16)
        two_columns(kernel_one, weight_one, depth)
        own_picture.wait()
        pick_rows(picture, field, margin_rows, images_in.shape[1], depth)
        relay(0)
        conv_one(field, weight_one, first, 1, first.shape[0] // unroll, unroll, depth, 1)

        @pl.when(side == 0)
        def _():
            picture[:, pl.ds(0, margin_rows)] = jnp.zeros(
                (images_in.shape[0], margin_rows, images_in.shape[2]), picture.dtype
            )

        @pl.when(side == 1)
        def _():
            sent_margin.wait_recv()

        pick_rows(picture, field, 0, margin_rows, depth)
        conv_one(field, weight_one, first, 0, 1, unroll, depth, 1)
        step(0)
        conv_two(first, kernel_two, second, 8)
        fetches[0].wait()
        chunk_three = largest_divisor(third.shape[1], 16)

        def act_three(row):
            made = conv_later(second, kernel_three, chunk_three, row)
            keep(third, row, chunk_three, third.shape[2], made.astype(jnp.float32))

        row_chunks(third.shape[1], chunk_three, act_three)
        fetches[1].wait()
        columns = third.shape[2] // 2

        def act_four(index, carry):
            made = conv_later(third, kernel_four, flat_rows // columns, index * (flat_rows // columns))
            there = pl.ds(pl.multiple_of(index * flat_rows, flat_rows), flat_rows)
            flat[side, there] = made
            flat_copy(side, index).start()
            return carry

        lax.fori_loop(0, flat_parts, act_four, 0)

    out_rows = images_in.shape[1] // 16
    counts = [(((out_rows * 2 + 1) * 2 + 1) * 2 + 1), (out_rows * 2 + 1) * 2 + 1, out_rows * 2 + 1]
    pairs = images_in.shape[2] // 4
    pl.run_scoped(
        stem,
        pltpu.VMEM((picture.shape[1] * depth, pairs), jnp.float32),
        pltpu.VMEM((3 * depth, 2 * kernel_two.shape[2]), jnp.float32),
        pltpu.VMEM((counts[0], pairs, 2 * kernel_two.shape[2]), jnp.bfloat16),
        pltpu.VMEM((kernel_two.shape[3] // LANES, counts[1], pairs, LANES), jnp.float32),
        pltpu.VMEM((kernel_three.shape[3] // LANES, counts[2], pairs // 2, LANES), jnp.float32),
    )
    step(1)
    out_cross = misc(wout.at[:, :, core], wout_other.at[:, :, core], 2, xpeer)
    out_cross.start()

    def embed(where, index):
        own = pl.ds(pl.multiple_of(index * half, half), half)
        chunk = (
            jnp.dot(flat[where, own], proj[...], preferred_element_type=jnp.float32)
            + pos[where, own].astype(jnp.float32)
        ).astype(jnp.bfloat16)
        tokens[where, own] = chunk
        normed[where, own] = norm_rows(chunk, gain_one[...])

    fetches[2].wait()
    fetches[3].wait()
    embed(side, 0)
    embed(side, 1)
    arriving = pos.at[other, piece]
    misc(arriving, arriving, 1, xpeer).wait_recv()
    pos_mirror = misc(arriving, arriving, 3, sibling)
    pos_mirror.start()
    step(2)
    coming = pos.at[other, other_piece]
    misc(coming, coming, 3, sibling).wait_recv()
    for index in range(flat_parts):
        flat_copy(other, index).wait_recv()
    embed(other, 0)
    embed(other, 1)
    step(3)

    cross = wout_other.at[:, :, core]
    out_mirror = misc(cross, cross, 4, sibling)

    def attention(qkv):
        def project(which):
            chunks[1 + which].ready()

            def act(where, carry):
                weight = wqkv[which].reshape(width, heads * head_size)
                made = pair_dot(weight, normed[where], ((0,), (1,)))
                columns = pl.ds(pl.multiple_of(where * rows, rows), rows)
                qkv[which, :, :, columns] = made.astype(jnp.bfloat16).reshape(heads, head_size, rows)
                return carry

            lax.fori_loop(0, 2, act, 0)

        project(0)
        project(1)
        step(4)
        project(2)
        factor = math.log2(math.e) / math.sqrt(head_size)

        def attend_head(index, carry):
            group, head = index // heads, index % heads
            keys, values = qkv[1, head], qkv[2, head]
            for where in range(2):
                columns = pl.ds(pl.multiple_of(where * rows + group * half, half), half)
                query = qkv[0, head, :, columns]
                score = pair_dot(keys, query, ((0,), (0,)))
                top = jnp.max(score, axis=0, keepdims=True)
                weight = jnp.exp2((score - top) * factor)
                below = jnp.sum(weight, axis=0, keepdims=True)
                made = jnp.dot(values, weight.astype(jnp.bfloat16), preferred_element_type=jnp.float32)
                made = (made / below).astype(jnp.bfloat16)
                mixed[side, group, head, :, where * half : (where + 1) * half] = made
            mix_copy(side, index).start()

            @pl.when(index == heads // 2 - 1)
            def _():
                misc(cross, cross, 2, xpeer).wait_recv()
                out_mirror.start()

            for number, when in PLACED:
                @pl.when(index == heads * when // 8)
                def _():
                    step(number)

            return carry

        lax.fori_loop(0, 2 * heads, attend_head, 0)

    def mix_copy(share_of, index):
        there = mixed.at[share_of, index // heads, index % heads]
        return remote(there, there, mix_send.at[index], mix_recv.at[index], xpeer)

    pl.run_scoped(attention, pltpu.VMEM((3, heads, head_size, count), jnp.bfloat16))
    mirror(4)
    mirror(5)
    forward(last_chunk + 1)
    mirror(last_chunk)
    chunks[0].ready()
    cross_other = wout_other.at[:, :, 1 - core]
    misc(cross_other, cross_other, 4, sibling).wait_recv()

    def settle(index, carry):
        group, where = index // 2, index % 2
        own = pl.ds(pl.multiple_of(group * half, half), half)
        columns = pl.ds(pl.multiple_of(where * half, half), half)
        attn = tokens[where, own].astype(jnp.float32)
        for share_of, weight in ((side, wout), (other, wout_other)):
            left = mixed[share_of, group, :, :, columns].reshape(heads * head_size, half)
            share = pair_dot(left, weight[...].reshape(width, heads * head_size), ((0,), (1,)))
            attn = attn + share.astype(jnp.bfloat16).astype(jnp.float32)
        chunk = attn.astype(jnp.bfloat16)
        tokens[where, own] = chunk
        normed[where, own] = norm_rows(chunk, gain_two[...])
        return carry

    slab_rows = width // line

    def back_copy(slab, group):
        there = pl.ds(pl.multiple_of(slab * slab_rows, slab_rows), slab_rows)
        lanes = pl.ds(group * half, half)
        return remote(
            back.at[there, lanes], arrived.at[there, lanes],
            back_send.at[slab, group], back_recv.at[slab, group], xpeer,
        )

    def feed(hidden, total):
        def rise(group):
            own = pl.ds(group * half, half)

            def act(quarter, carry):
                weight = wup[quarter].reshape(width, part)
                before = jnp.dot(
                    normed[:, own].reshape(2 * half, width), weight, preferred_element_type=jnp.float32
                )
                made = 0.5 * before * (1.0 + lax.erf(before * math.sqrt(0.5)))
                there = pl.ds(pl.multiple_of(quarter * part, part), part)
                hidden[:, own, there] = made.astype(jnp.bfloat16).reshape(2, half, part)
                return carry

            lax.fori_loop(0, quarters, act, 0)

        def weight_of(order):
            slab = slab_at(order)
            there = pl.ds(pl.multiple_of(slab * slab_rows, slab_rows), slab_rows)
            return slab, there, wdown[slab].reshape(slab_rows, units)

        def give(order, group):
            slab, there, weight = weight_of(order)
            own = pl.ds(group * half, half)
            back[there, own] = pair_dot(weight, hidden[other, own], ((1,), (1,))).astype(jnp.bfloat16)
            back_copy(slab, group).start()

        def fall(order):
            slab, there, weight = weight_of(order)
            total[there] = pair_dot(weight, hidden[side], ((1,), (1,))).astype(jnp.bfloat16)

        def meet(group):
            for head in range(heads):
                mix_copy(other, group * heads + head).wait_recv()
            lax.fori_loop(2 * group, 2 * group + 2, settle, 0)

        mirror(6)
        mirror(7)
        meet(0)
        relay(last_chunk)
        forward(last_chunk + 2)
        for quarter in range(quarters):
            chunks[4 + quarter].ready()
        rise(0)
        down.ready(slab_at(0))
        give(0, 0)
        mirror(last_chunk + 1)
        down.ready(slab_at(1))
        give(1, 0)
        forward(last_chunk + 3)
        meet(1)
        rise(1)
        mirror(last_chunk + 2)
        give(0, 1)
        give(1, 1)
        fall(0)
        down.ready(slab_at(2))
        give(2, 0)
        give(2, 1)
        for order in range(4, line):
            forward(last_chunk + order)
        fall(1)
        for order in range(3, line):
            mirror(last_chunk + order)
        for order in range(3, line):
            down.ready(slab_at(order))
            give(order, 0)
            give(order, 1)
        for order in range(2, line):
            fall(order)
        for slab in range(line):
            for group in range(2):
                back_copy(slab, group).wait_recv()
        summed = total[...].astype(jnp.float32) + arrived[...].astype(jnp.float32)
        encoded[...] = (tokens[side].astype(jnp.float32) + summed.T).astype(jnp.bfloat16)

    pl.run_scoped(
        feed, pltpu.VMEM((2, rows, units), jnp.bfloat16), pltpu.VMEM((width, rows), jnp.bfloat16)
    )

    @pl.when(side == 0)
    def _():
        sent_margin.wait_send()

    for copy in (pos_send, out_cross, pos_mirror, out_mirror):
        copy.wait_send()
    for index in range(flat_parts):
        flat_copy(side, index).wait_send()
    for index in range(2 * heads):
        mix_copy(side, index).wait_send()
    for slab in range(line):
        for group in range(2):
            back_copy(slab, group).wait_send()
    for chunk in chunks:
        chunk.drain()
    down_line.drain_line()
    down.drain()


def whole_block(
    images, pos, kernel_one, kernel_two, kernel_three, kernel_four, proj, gain_one, gain_two,
    qkv_shard, out_shard, up_shard, down_shard,
):
    line = lax.axis_size("dp") // 4
    depth, local, units = qkv_shard.shape[1], qkv_shard.shape[2], up_shard.shape[1]
    rows, width = pos.shape
    head_size = width // HEADS
    heads = local // head_size
    quarters = 4
    numbers = 5 + quarters + len(PAIRED)
    whole = 4 + quarters
    here = (line, 2, 2, depth)
    bf16 = jnp.bfloat16
    vmem = pl.BlockSpec(memory_space=pltpu.VMEM)
    hbm = pl.BlockSpec(memory_space=pl.ANY)
    dma = pltpu.SemaphoreType.DMA
    return pl.pallas_call(
        functools.partial(block_body, line, head_size),
        out_shape=jax.ShapeDtypeStruct((rows, width), bf16),
        in_specs=[hbm, vmem, vmem, hbm, hbm, hbm, hbm, vmem, vmem, hbm, hbm, hbm, hbm],
        out_specs=vmem,
        scratch_shapes=[
            pltpu.VMEM((images.shape[1], images.shape[2] + 16, images.shape[3]), bf16),
            pltpu.VMEM(kernel_three.shape, bf16),
            pltpu.VMEM(kernel_four.shape, bf16),
            pltpu.VMEM(proj.shape, bf16),
            pltpu.VMEM((2, rows, proj.shape[0]), bf16),
            pltpu.VMEM((2, rows, width), bf16),
            pltpu.VMEM((2, rows, width), bf16),
            pltpu.VMEM((2, rows, width), bf16),
            pltpu.VMEM((3, *here, local), bf16),
            pltpu.VMEM((*here, local), bf16),
            pltpu.VMEM((*here, local), bf16),
            pltpu.VMEM((quarters, *here, units // quarters), bf16),
            pltpu.VMEM((*here, units), bf16),
            pltpu.VMEM((2, 2, heads, head_size, rows), bf16),
            pltpu.VMEM((width, rows), bf16),
            pltpu.VMEM((width, rows), bf16),
            dma((numbers, 4 + 2 * (line - 3))),
            dma((numbers, line)),
            dma((whole,)),
            dma((whole,)),
            dma((whole,)),
            dma((whole,)),
            dma((whole,)),
            dma((3,)),
            dma((line,)),
            dma((line,)),
            dma((7,)),
            dma((7,)),
            dma((5,)),
            dma((2 * heads,)),
            dma((2 * heads,)),
            dma((line, 2)),
            dma((line, 2)),
        ],
        compiler_params=pltpu.CompilerParams(
            collective_id=0, has_side_effects=True, vmem_limit_bytes=VMEM_LIMIT
        ),
    )(
        images[0], kernel_one, kernel_two, kernel_three, kernel_four, pos, proj, gain_one, gain_two,
        qkv_shard, out_shard, up_shard, down_shard,
    )


def on_ring(
    images,
    pos_embed,
    conv_first,
    conv_second,
    conv_third,
    conv_fourth,
    proj_weight,
    ln_first,
    qkv_weight,
    out_weight,
    ln_second,
    up_weight,
    down_weight,
):
    count = lax.axis_size("space")
    attention_part = gathered(
        jnp.concatenate([jnp.moveaxis(qkv_weight, 1, 0), out_weight.T[None]], axis=0), 1
    )
    feed_part = gathered(jnp.stack([up_weight, down_weight.T]), 1)
    out_part = attention_part[3]
    up_part, down_part = feed_part[0], feed_part[1]
    margin = passed_along(images[:, :, -15:, :], "space", 1)
    positions = [pos_embed] + [shifted(pos_embed, "space", k) for k in range(1, count)]

    stem_out = second_conv(first_conv(images, margin, conv_first), conv_second)
    for kernel in (conv_third, conv_fourth):
        stem_out = later_conv(stem_out, kernel)
    flat = stem_out.reshape(-1, stem_out.shape[3])
    flats = [flat] + [shifted(flat, "space", k) for k in range(1, count)]
    width = proj_weight.shape[1]
    local = attention_part.shape[2]
    head_size = width // HEADS

    tokens = None
    projected = []
    for rows, position in zip(flats, positions):
        chunk = (
            jnp.dot(rows, proj_weight, preferred_element_type=jnp.float32)
            + position.astype(jnp.float32)
        ).astype(jnp.bfloat16)
        tokens = chunk if tokens is None else tokens
        normed = layer_norm(chunk, ln_first)
        projected.append(
            [
                lax.dot_general(
                    attention_part[which],
                    normed,
                    (((0,), (1,)), ((), ())),
                    preferred_element_type=jnp.float32,
                ).astype(jnp.bfloat16)
                for which in range(3)
            ]
        )
    keys = [part[1] for part in projected]
    values = [part[2] for part in projected]

    def attention_share(query):
        mixed = attend(query, keys, values, head_size)
        share = lax.dot_general(
            mixed, out_part, (((0,), (1,)), ((), ())), preferred_element_type=jnp.float32
        ).astype(jnp.bfloat16)
        return mixed, share

    returned = []
    last = None
    for k in list(range(1, count)) + [0]:
        query = projected[k][0]
        if last is not None:
            query, _ = lax.optimization_barrier((query, last))
        last, share = attention_share(query)
        returned.append(shifted(share, "space", -k) if k else share)
    attn_sum = sum(part.astype(jnp.float32) for part in returned)
    after_attn = (tokens.astype(jnp.float32) + attn_sum).astype(jnp.bfloat16)
    normed_two = layer_norm(after_attn, ln_second)

    def feed_forward(rows):
        before = jnp.dot(rows, up_part, preferred_element_type=jnp.float32)
        hidden = (0.5 * before * (1.0 + lax.erf(before * math.sqrt(0.5)))).astype(jnp.bfloat16)
        hidden = lax.optimization_barrier(hidden)
        return lax.dot_general(
            hidden, down_part, (((1,), (1,)), ((), ())), preferred_element_type=jnp.float32
        ).astype(jnp.bfloat16)

    rows = normed_two.shape[0]
    half = rows // 2
    pieces = [normed_two[:half], normed_two[half:]]
    moved = [[shifted(piece, "space", k) for piece in pieces] for k in range(1, count)]
    totals = feed_forward(normed_two).astype(jnp.float32)
    back = [
        jnp.concatenate([shifted(feed_forward(piece), "space", -k) for piece in there], axis=0)
        for k, there in zip(range(1, count), moved)
    ]
    for part in back:
        totals = totals + part.astype(jnp.float32)
    return (after_attn.astype(jnp.float32) + totals).astype(jnp.bfloat16)[None]


def on_device(
    images,
    pos_embed,
    conv_first,
    conv_second,
    conv_third,
    conv_fourth,
    proj_weight,
    ln_first,
    qkv_weight,
    out_weight,
    ln_second,
    up_weight,
    down_weight,
):
    shards = lax.axis_size("dp")
    fits = lax.axis_size("space") == 2 and shards % 16 == 0 and images.shape[0] == 1
    fits = fits and qkv_weight.shape[0] % 16 == 0 and qkv_weight.shape[2] % 128 == 0
    if not fits:
        return on_ring(
            images, pos_embed, conv_first, conv_second, conv_third, conv_fourth, proj_weight,
            ln_first, qkv_weight, out_weight, ln_second, up_weight, down_weight,
        )
    out = whole_block(
        images, pos_embed, conv_first, conv_second, conv_third, conv_fourth, proj_weight,
        ln_first, ln_second,
        jnp.moveaxis(qkv_weight, 1, 0), out_weight.T, up_weight, down_weight.T,
    )
    return out[None]


def solution(mesh):
    placed = (
        P("dp", None, "space", None),
        P("space", None),
        P(),
        P(),
        P(),
        P(),
        P(),
        P(),
        P("dp", None, "space"),
        P("space", "dp"),
        P(),
        P("dp", "space"),
        P("space", "dp"),
    )
    return jax.shard_map(
        on_device, mesh=mesh, in_specs=placed, out_specs=P("dp", "space", None), check_vma=False
    )
```
